256 devices in a mesh: ctx: 128 (over x, y_hi, z, core), head: 2 (over y_lo).
Axes of the slice: x: 4, y: 4 (y_hi: 2, y_lo: 2; y = y_hi * 2 + y_lo), z: 8, core: 2. Of those that a mesh axis runs over, the one named last changes fastest.
Arguments:
- queries: bfloat16 [16384, 2048], P('ctx', 'head'), may hold values from -160 to 160
- rotated_keys: bfloat16 [16384, 512], P('ctx', 'head'), may hold values from -6 to 6
- value_matrix: bfloat16 [16384, 512], P('ctx', 'head'), may hold values from -6 to 6
- doc_lengths: int32 [8], replicated, may hold values from 1 to 12288, 16384 in all
- scored: int32 [512], P('ctx'), may hold values from 0 to 127, as said below
- residual: bfloat16 [512, 4096], P('ctx', 'head'), may hold values from -18 to 18
- norm_gain: float32 [4096], P('head'), may hold values from 0.5 to 1.5
- out_weight: bfloat16 [2048, 4096], P('head'), may hold values from -0.5 to 0.5
- lm_weight: bfloat16 [4096, 128256], P('head', 'ctx'), may hold values from -0.40625 to 0.40625
- token_ids: int32 [512], replicated, may hold values from 0 to 128255
- old_logp: float32 [512], replicated, may hold values from -24 to -9
- advantage: float32 [512], replicated, may hold values from -3 to 3
Outputs:
- attended: bfloat16 [16384, 2048], P('ctx', 'head')
- log_probs: float32 [512], replicated
- token_loss: float32 [512], replicated
The draws below stay inside these ranges and needn't reach their ends.
Inputs may be any that keep to these rules, and one draw needn't show every extreme that they name: `scored`: each aligned block of 4 entries holds distinct increasing offsets. `doc_lengths`: the longest document has exactly three quarters of 16384 positions.
All inputs are finite; a program needn't handle non-finite values.
Results may differ from the reference program's by a relative error of at most 0.0065.
Values may be sent and summed in bfloat16 or wider, within the bound.
No kernel may reach another device: no remote copies, remote signals or barrier semaphores. Data moves between devices by JAX's collectives and lax.ppermute only.
A program may use at most 128 MiB of HBM per device.

```python
import math
import jax
import jax.numpy as jnp
import numpy as np
from jax import lax

D = 4096
QUERY_HEADS = 16
KEY_VALUE_HEADS = 4
HEAD_SIZE = 128
V = 128256
TOK_DEV = 128
RESP_DEV = 4
DOCS = 8
PACKED_LENGTH = 16384
RESP = 512


def key_sample(key):
    drawn_sample = jax.random.normal(jax.random.fold_in(key, 12), (PACKED_LENGTH, KEY_VALUE_HEADS * HEAD_SIZE), jnp.float32)
    return jnp.clip(drawn_sample, -6.0, 6.0)


def draw_rotated_keys(key, part):
    sample = key_sample(key)
    return sample.astype(jnp.bfloat16)


def draw_queries(key, part):
    sample = 2.0 * jnp.clip(jax.random.normal(jax.random.fold_in(key, 11), (PACKED_LENGTH, QUERY_HEADS * HEAD_SIZE), jnp.float32), -6.0, 6.0)
    return sample.astype(jnp.bfloat16)


def draw_lm_weight(key, part):
    weight_scale = 3.0 * D ** (-0.5)
    sample = jnp.clip(jax.random.normal(jax.random.fold_in(key, 23), (D, V), jnp.float32), -6.0, 6.0) * weight_scale
    return sample.astype(jnp.bfloat16)


def column_scales():
    steps = jnp.arange(D, dtype=jnp.float32) / max(D - 1, 1)
    return jnp.exp(jnp.log(0.5) + steps * jnp.log(5.9))


def draw_residual(key, part):
    widths = column_scales()[None, :]
    sample = jnp.clip(jax.random.normal(jax.random.fold_in(key, 24), (RESP, D), jnp.float32), -6.0, 6.0) * widths
    return sample.astype(jnp.bfloat16)


def draw_scored(key, part):

    def one_block(block_index):
        picked = jax.random.permutation(jax.random.fold_in(key, block_index), TOK_DEV)[:RESP_DEV]
        return jnp.sort(picked)
    return jax.vmap(one_block)(jnp.arange(RESP // RESP_DEV)).reshape(RESP).astype(jnp.int32)


def with_ends(values, own_key, least, top_value):
    spot = [jax.random.randint(jax.random.fold_in(own_key, axis), (), 0, length) for axis, length in enumerate(values.shape)]
    main_axis = values.shape.index(max(values.shape))
    neighbour = spot[:main_axis] + [(spot[main_axis] + 1) % values.shape[main_axis]] + spot[main_axis + 1:]
    return values.at[tuple(spot)].set(least).at[tuple(neighbour)].set(top_value)


def block_scale(stream_key, shape, split, low, high):
    gain = 1.0
    for dim, blocks in split:
        heights = jax.random.uniform(jax.random.fold_in(jax.random.fold_in(stream_key, 6), dim), (blocks,), jnp.float32, low / len(split), high / len(split))
        gain = gain * jnp.repeat(jnp.exp(heights), shape[dim] // blocks).reshape((-1,) + (1,) * (len(shape) - 1 - dim))
    return gain


def skewed_wide(own_key, extent, number_of, lean):
    weights = [min(1 << octave, number_of + 1 - (1 << octave)) * (1 << 20) // math.isqrt((1 << octave) ** lean) + 1 for octave in range((number_of + 1).bit_length()) if 1 << octave <= number_of]
    width = 1 + sum(weights) // (1 << 30)
    table = np.cumsum(np.array([max(1, weight // width) for weight in weights]))
    lot = jax.random.randint(jax.random.fold_in(own_key, 1), extent, 0, int(table[len(weights) - 1]))
    start = jnp.left_shift(1, jnp.searchsorted(jnp.asarray(table, jnp.int32), lot, side="right").astype(jnp.int32))
    grade = start - 1 + jax.random.randint(jax.random.fold_in(own_key, 4), extent, 0, 1 << 30) % jnp.minimum(start, number_of + 1 - start)
    return jax.random.permutation(jax.random.fold_in(own_key, 2), number_of)[grade].astype(jnp.int32)


def length_profile(number_of, total, bound, skew):
    weights = [(1 << 20) // math.isqrt(grade ** skew) + 1 for grade in range(2, number_of + 1)]
    spare, holding = total - bound - (number_of - 1), [1] * (number_of - 1)
    while spare > 0:
        candidates = [i for i in range(number_of - 1) if holding[i] < bound]
        mass, budget = sum([weights[i] for i in candidates]), spare
        for i in candidates:
            addition = min(bound - holding[i], max(1, budget * weights[i] // mass), spare)
            holding[i] = holding[i] + addition
            spare = spare - addition
    return np.array([bound] + holding)


def ragged_sizes(own_key, count, total, limit, lean):
    if count == 2:
        one = jax.random.randint(own_key, (), max(1, total - limit), min(limit, total - 1) + 1)
        return jnp.stack([one, total - one])
    sizes = jnp.asarray(length_profile(count, total, limit, lean), jnp.int32)
    twos = (count - 1) // 2
    source_of, receiver = sizes[1:1 + 2 * twos:2], sizes[2:2 + 2 * twos:2]
    margin = jnp.minimum(source_of - 1, limit - receiver)
    shifted = jax.random.randint(jax.random.fold_in(own_key, 1), (twos,), 0, 1 << 20) % (margin + 1)
    sizes = sizes.at[1:1 + 2 * twos:2].set(source_of - shifted).at[2:2 + 2 * twos:2].set(receiver + shifted)
    return sizes[jax.random.permutation(jax.random.fold_in(own_key, 2), count)]


def centred(rng, extent, deviation, limit, pieces=(), kind=jnp.bfloat16):
    entries = deviation * jax.random.normal(rng, extent, jnp.float32)
    if pieces:
        entries = entries * block_scale(rng, extent, pieces, -0.22, 0.18)
    return jnp.clip(entries, -limit, limit).astype(kind)


def setup_inputs(seed: int = 0) -> dict:
    keys = jax.random.split(jax.random.key(seed), 13)
    return {
        "queries": draw_queries(jax.random.fold_in(keys[12], 71), 0),
        "rotated_keys": draw_rotated_keys(jax.random.fold_in(keys[12], 71), 0),
        "value_matrix": centred(keys[2], (PACKED_LENGTH, KEY_VALUE_HEADS * HEAD_SIZE), 1.0, 6.0, ((0, 128), (1, 2))),
        "doc_lengths": ragged_sizes(keys[3], DOCS, PACKED_LENGTH, 3 * PACKED_LENGTH // 4, 2).astype(jnp.int32),
        "scored": draw_scored(jax.random.fold_in(keys[12], 71), 0),
        "residual": draw_residual(jax.random.fold_in(keys[12], 71), 0),
        "norm_gain": jnp.clip(1.0 + 0.1 * jax.random.normal(keys[6], (D,), jnp.float32), 0.5, 1.5),
        "out_weight": centred(keys[7], (QUERY_HEADS * HEAD_SIZE, D), (QUERY_HEADS * HEAD_SIZE // 16) ** -0.5, 0.5, ((0, 2),)),
        "lm_weight": draw_lm_weight(jax.random.fold_in(keys[12], 71), 0),
        "token_ids": with_ends(skewed_wide(keys[9], (RESP,), V, 2), jax.random.fold_in(keys[9], 3), 0, V - 1).astype(jnp.int32),
        "old_logp": jnp.clip(jax.random.uniform(keys[10], (RESP,), jnp.float32, -24.0, -9.0), -24.0, -9.0),
        "advantage": centred(keys[11], (RESP,), 0.5, 3.0, (), jnp.float32),
    }


def doc_index(positions, doc_ends):
    return lax.optimization_barrier(jnp.sum((positions[:, None] >= doc_ends[None, :]).astype(jnp.int32), axis=1))

def reference(queries, rotated_keys, value_matrix, doc_lengths, scored, residual, norm_gain, out_weight, lm_weight, token_ids, old_logp, advantage):
    group_count = QUERY_HEADS // KEY_VALUE_HEADS
    doc_ends = jnp.cumsum(doc_lengths).astype(jnp.int32)
    key_pos = jnp.arange(PACKED_LENGTH, dtype=jnp.int32)
    key_doc = doc_index(key_pos, doc_ends)
    key_head_rows = rotated_keys.reshape(PACKED_LENGTH, KEY_VALUE_HEADS, HEAD_SIZE).astype(jnp.float32)
    value_head_rows = value_matrix.reshape(PACKED_LENGTH, KEY_VALUE_HEADS, HEAD_SIZE).astype(jnp.float32)
    query_matrix = min(256, PACKED_LENGTH)

    def one_block(offset):
        block_tile = lax.dynamic_slice_in_dim(queries, offset, query_matrix, 0)
        block_tile = block_tile.reshape(query_matrix, KEY_VALUE_HEADS, group_count, HEAD_SIZE).astype(jnp.float32)
        scores = jnp.einsum('qkgd,rkd->kgqr', block_tile, key_head_rows) * HEAD_SIZE ** (-0.5)
        query_pos = offset + jnp.arange(query_matrix, dtype=jnp.int32)
        allowed = (key_pos[None, :] <= query_pos[:, None]) & (key_doc[None, :] == doc_index(query_pos, doc_ends)[:, None])
        scores = jnp.where(allowed, scores, -1e+30)
        row_top = lax.optimization_barrier(jnp.max(scores, axis=-1, keepdims=True))
        weights = jnp.where(allowed, jnp.exp(scores - row_top), 0.0)
        row_total = lax.optimization_barrier(jnp.sum(weights, axis=-1, keepdims=True))
        probs = lax.optimization_barrier(weights.astype(jnp.bfloat16)).astype(jnp.float32)
        result = jnp.einsum('kgqr,rkd->kgqd', probs, value_head_rows) / row_total
        return jnp.transpose(result, (2, 0, 1, 3)).reshape(query_matrix, QUERY_HEADS * HEAD_SIZE).astype(jnp.bfloat16)
    offsets = jnp.arange(PACKED_LENGTH // query_matrix, dtype=jnp.int32) * query_matrix
    attended = lax.map(one_block, offsets).reshape(PACKED_LENGTH, QUERY_HEADS * HEAD_SIZE)
    positions = jnp.arange(RESP, dtype=jnp.int32) // RESP_DEV * TOK_DEV + scored
    chosen = jnp.take(attended, positions, axis=0)
    hidden = residual.astype(jnp.float32) + jnp.dot(chosen, out_weight, preferred_element_type=jnp.float32)
    mean_square = lax.optimization_barrier(jnp.mean(hidden * hidden, axis=1, keepdims=True))
    normed = (hidden * lax.rsqrt(mean_square + 1e-05) * norm_gain[None, :]).astype(jnp.bfloat16)
    logits = jnp.dot(normed, lm_weight, preferred_element_type=jnp.float32)
    row_top = lax.optimization_barrier(jnp.max(logits, axis=1))
    row_total = lax.optimization_barrier(jnp.sum(jnp.exp(logits - row_top[:, None]), axis=1))
    target = jnp.take_along_axis(logits, token_ids[:, None].astype(jnp.int32), axis=1)[:, 0]
    log_probs = target - row_top - jnp.log(row_total)
    ratio = jnp.exp(jnp.clip(log_probs - old_logp, -4.0, 4.0))
    token_loss = -jnp.minimum(ratio * advantage, jnp.clip(ratio, 0.8, 1.2) * advantage)
    return (attended, log_probs, token_loss)
```

```python
import functools

import jax
import jax.numpy as jnp
from jax import lax
from jax.experimental import pallas as pl
from jax.experimental.pallas import tpu as pltpu
from jax.sharding import Mesh
from jax.sharding import PartitionSpec as P

HEAD_SIZE = 128
GROUP = 4
DOCS = 8
AXES = ("ctx_0", "ctx_1", "ctx_2", "ctx_3", "head")
XYC = ("ctx_0", "ctx_1", "ctx_3")
XY = ("ctx_0", "ctx_1")
ZC = ("ctx_2", "ctx_3")
XYCH = ("ctx_0", "ctx_1", "ctx_3", "head")

LOG2E = 1.4426950408889634
SCORE_TO_LOG2 = HEAD_SIZE ** (-0.5) * LOG2E
MASKED = -1e30
NO_TOP = -1e20
KEY_BLOCK = 512


def size_of(axes):
    n = 1
    for a in axes:
        n *= lax.axis_size(a)
    return n


def spread(shard, axes):
    n = size_of(axes)
    return lax.all_to_all(
        jnp.broadcast_to(shard[None], (n, *shard.shape)), axes, 0, 0, tiled=True
    )


def swap_heads(shard):
    return lax.ppermute(shard, "head", [(0, 1), (1, 0)])


def attention_kernel(meta_ref, q_ref, kv_ref, out_ref, v_ref, m_ref, acc_ref):
    j = pl.program_id(0)
    keys = kv_ref.shape[0]
    rows = q_ref.shape[0] * q_ref.shape[1]

    @pl.when(j == 0)
    def _():
        v_ref[:, :HEAD_SIZE] = kv_ref[:, HEAD_SIZE:]
        v_ref[:, HEAD_SIZE:] = jnp.ones((keys, HEAD_SIZE), jnp.bfloat16)

    first_q = meta_ref[DOCS] + j * meta_ref[DOCS + 1]
    last_q = first_q + rows - 1
    first_k = meta_ref[DOCS + 2]

    def start_of(pos):
        low = jnp.int32(0)
        for d in range(DOCS):
            start = meta_ref[d]
            low = jnp.where(start <= pos, jnp.maximum(low, start), low)
        return low

    low_first = start_of(first_q)
    low_last = start_of(last_q)
    m_ref[...] = jnp.full(m_ref.shape, NO_TOP, jnp.float32)
    acc_ref[...] = jnp.zeros(acc_ref.shape, jnp.float32)
    block_lo = jnp.maximum(low_first - first_k, 0) // KEY_BLOCK
    block_hi = jnp.clip(last_q - first_k + KEY_BLOCK, 0, keys) // KEY_BLOCK

    def attend(b, masked):
        at = pl.multiple_of(b * KEY_BLOCK, KEY_BLOCK)
        k = kv_ref[pl.ds(at, KEY_BLOCK), :HEAD_SIZE]
        v = v_ref[pl.ds(at, KEY_BLOCK), :]
        if masked:
            pos = first_q + lax.broadcasted_iota(jnp.int32, (rows, 1), 0)
            low = jnp.zeros((rows, 1), jnp.int32)
            for d in range(DOCS):
                start = meta_ref[d]
                low = jnp.where(start <= pos, jnp.maximum(low, start), low)
            base = first_k + at
            key = lax.broadcasted_iota(jnp.int32, (rows, KEY_BLOCK), 1)
            allowed = (key >= low - base) & (key <= pos - base)
        for g in range(GROUP):
            q = q_ref[:, :, g * HEAD_SIZE : (g + 1) * HEAD_SIZE].reshape(rows, HEAD_SIZE)
            s = lax.dot_general(
                q, k, (((1,), (1,)), ((), ())), preferred_element_type=jnp.float32
            )
            if masked:
                s = jnp.where(allowed, s, MASKED)
            m_old = m_ref[g]
            m_new = jnp.maximum(
                m_old, jnp.max(s, axis=1, keepdims=True) * SCORE_TO_LOG2
            )
            p = jnp.exp2(s * SCORE_TO_LOG2 - m_new[:, :1]).astype(jnp.bfloat16)
            update = jnp.dot(p, v, preferred_element_type=jnp.float32)
            rescale = jnp.exp2(m_old - m_new)
            acc_ref[g] = acc_ref[g] * rescale[:, :1] + update
            m_ref[g] = m_new

    def step(b, carry):
        block_first = first_k + b * KEY_BLOCK
        free = (block_first >= low_last) & (block_first + KEY_BLOCK - 1 <= first_q)

        @pl.when(free)
        def _():
            attend(b, False)

        @pl.when(jnp.logical_not(free))
        def _():
            attend(b, True)

        return carry

    lax.fori_loop(block_lo, block_hi, step, 0)
    lane = lax.broadcasted_iota(jnp.int32, (rows, HEAD_SIZE), 1)
    stats = jnp.zeros((rows, HEAD_SIZE), jnp.float32)
    for g in range(GROUP):
        total = acc_ref[g][:, HEAD_SIZE:]
        some = total > 0.0
        total = jnp.where(some, total, 1.0)
        result = acc_ref[g][:, :HEAD_SIZE] / total
        out_ref[:, :, g * HEAD_SIZE : (g + 1) * HEAD_SIZE] = result.astype(
            jnp.bfloat16
        ).reshape(2, rows // 2, HEAD_SIZE)
        level = jnp.where(some, m_ref[g] + jnp.log2(total), NO_TOP)
        high = level.astype(jnp.bfloat16).astype(jnp.float32)
        rest = level - high
        middle = rest.astype(jnp.bfloat16).astype(jnp.float32)
        low = rest - middle
        stats = jnp.where(lane == g, high, stats)
        stats = jnp.where(lane == GROUP + g, middle, stats)
        stats = jnp.where(lane == 2 * GROUP + g, low, stats)
    out_ref[:, :, GROUP * HEAD_SIZE :] = stats.astype(jnp.bfloat16).reshape(
        2, rows // 2, HEAD_SIZE
    )


def partial_attention(meta, q_all, kv_all):
    blocks, half, width = q_all.shape
    keys = kv_all.shape[0]
    rows = 2 * half
    return pl.pallas_call(
        attention_kernel,
        grid_spec=pltpu.PrefetchScalarGridSpec(
            num_scalar_prefetch=1,
            grid=(blocks // 2,),
            in_specs=[
                pl.BlockSpec((2, half, width), lambda j, meta: (j, 0, 0)),
                pl.BlockSpec((keys, 2 * HEAD_SIZE), lambda j, meta: (0, 0)),
            ],
            out_specs=pl.BlockSpec((2, half, width + HEAD_SIZE), lambda j, meta: (j, 0, 0)),
            scratch_shapes=[
                pltpu.VMEM((keys, 2 * HEAD_SIZE), jnp.bfloat16),
                pltpu.VMEM((GROUP, rows, HEAD_SIZE), jnp.float32),
                pltpu.VMEM((GROUP, rows, 2 * HEAD_SIZE), jnp.float32),
            ],
        ),
        out_shape=jax.ShapeDtypeStruct((blocks, half, width + HEAD_SIZE), jnp.bfloat16),
        compiler_params=pltpu.CompilerParams(dimension_semantics=("arbitrary",)),
        name="partial_attention",
    )(meta, q_all, kv_all)


def merge_kernel(scored_ref, parts_ref, attended_ref, chosen_ref):
    windows = parts_ref.shape[0] // 2
    rows = parts_ref.shape[1]
    for c in range(2):
        levels = []
        for w in range(windows):
            st = parts_ref[2 * w + c, :, GROUP * HEAD_SIZE :].astype(jnp.float32)
            levels.append(
                st
                + pltpu.roll(st, HEAD_SIZE - GROUP, 1)
                + pltpu.roll(st, HEAD_SIZE - 2 * GROUP, 1)
            )
        top = functools.reduce(jnp.maximum, levels)
        shares = [jnp.exp2(level - top) for level in levels]
        total = functools.reduce(jnp.add, shares)
        shares = [share / total for share in shares]
        for g in range(GROUP):
            result = jnp.zeros((rows, HEAD_SIZE), jnp.float32)
            for w in range(windows):
                part = parts_ref[2 * w + c, :, g * HEAD_SIZE : (g + 1) * HEAD_SIZE]
                result = result + shares[w][:, g : g + 1] * part.astype(jnp.float32)
            at = (c * GROUP + g) * HEAD_SIZE
            attended_ref[:, at : at + HEAD_SIZE] = result.astype(jnp.bfloat16)
    count = scored_ref.shape[0]
    row = lax.broadcasted_iota(jnp.int32, (chosen_ref.shape[0], rows), 0)
    col = lax.broadcasted_iota(jnp.int32, (chosen_ref.shape[0], rows), 1)
    pick = jnp.zeros((chosen_ref.shape[0], rows), jnp.float32)
    for i in range(count):
        pick = jnp.where((row == i) & (col == scored_ref[i]), 1.0, pick)
    chosen_ref[...] = jnp.dot(
        pick.astype(jnp.bfloat16), attended_ref[...], preferred_element_type=jnp.float32
    ).astype(jnp.bfloat16)


def merged_attention(scored, parts):
    rows = parts.shape[1]
    width = 2 * GROUP * HEAD_SIZE
    return pl.pallas_call(
        merge_kernel,
        in_specs=[
            pl.BlockSpec(memory_space=pltpu.SMEM),
            pl.BlockSpec(memory_space=pltpu.VMEM),
        ],
        out_specs=(
            pl.BlockSpec(memory_space=pltpu.VMEM),
            pl.BlockSpec(memory_space=pltpu.VMEM),
        ),
        out_shape=(
            jax.ShapeDtypeStruct((rows, width), jnp.bfloat16),
            jax.ShapeDtypeStruct((16, width), jnp.bfloat16),
        ),
        name="merged_attention",
    )(scored, parts)


def merged_stats(stats, axis):
    tops, sums, targets = stats
    top = jnp.max(tops, axis=axis)
    total = jnp.sum(sums * jnp.exp(tops - jnp.expand_dims(top, axis)), axis=axis)
    return (top, total, jnp.sum(targets, axis=axis))


def per_device(
    queries,
    rotated_keys,
    value_matrix,
    doc_lengths,
    scored,
    residual,
    norm_gain,
    out_weight,
    lm_weight,
    token_ids,
    old_logp,
    advantage,
):
    tok_rows = queries.shape[0]
    count = scored.shape[0]
    cores = lax.axis_size("ctx_3")
    window_count = size_of(XY)
    z_count = lax.axis_size("ctx_2")
    window = lax.axis_index(XY)
    z = lax.axis_index("ctx_2")
    chip_rows = cores * tok_rows
    window_rows = z_count * chip_rows

    doc_starts = jnp.cumsum(doc_lengths) - doc_lengths
    meta = jnp.concatenate(
        [
            doc_starts.astype(jnp.int32),
            jnp.stack([z * chip_rows, jnp.int32(window_rows), window * window_rows]).astype(
                jnp.int32
            ),
        ]
    )
    by_core = jnp.swapaxes(queries.reshape(tok_rows, cores, GROUP * HEAD_SIZE), 0, 1)
    q_send = jnp.broadcast_to(by_core[None], (window_count, *by_core.shape)).reshape(
        window_count * cores, tok_rows, GROUP * HEAD_SIZE
    )
    kv = jnp.concatenate(
        [
            rotated_keys.reshape(tok_rows, cores, HEAD_SIZE),
            value_matrix.reshape(tok_rows, cores, HEAD_SIZE),
        ],
        axis=2,
    )
    kv = jnp.swapaxes(kv, 0, 1)
    kv_send = jnp.broadcast_to(kv[None], (z_count, *kv.shape)).reshape(
        z_count * cores, tok_rows, 2 * HEAD_SIZE
    )
    kv_all = lax.all_to_all(kv_send, ZC, 0, 0, tiled=True).reshape(-1, 2 * HEAD_SIZE)
    q_all = lax.all_to_all(q_send, XYC, 0, 0, tiled=True)
    parts = partial_attention(meta, q_all, kv_all)
    arrived = lax.all_to_all(parts, XYC, 0, 0, tiled=True)
    attended, chosen = merged_attention(scored, arrived)

    half = residual.shape[1]
    head = lax.axis_index("head")
    partial_value = jnp.dot(chosen, out_weight, preferred_element_type=jnp.float32)[:count]
    own = lax.dynamic_slice_in_dim(partial_value, head * half, half, 1)
    own = own + residual.astype(jnp.float32)
    partial_value = lax.dynamic_update_slice_in_dim(partial_value, own, head * half, 1)
    other = swap_heads(partial_value.astype(jnp.bfloat16)).astype(jnp.float32)
    hidden_all = partial_value + other
    squares = jnp.sum(hidden_all * hidden_all, axis=1, keepdims=True)
    hidden = own + lax.dynamic_slice_in_dim(other, head * half, half, 1)
    normed = (
        hidden * lax.rsqrt(squares / hidden_all.shape[1] + 1e-05) * norm_gain[None, :]
    ).astype(jnp.bfloat16)

    along_z = spread(normed, ("ctx_2",))
    along_xy = spread(along_z, XY)
    everyone = spread(along_xy, ("ctx_3",)).reshape(-1, half)
    row_count = everyone.shape[0]
    ids = token_ids.reshape(-1, cores, count).swapaxes(0, 1).reshape(row_count)
    partial_logits = jnp.dot(everyone, lm_weight, preferred_element_type=jnp.float32)
    rows = row_count // 2
    theirs = lax.dynamic_slice_in_dim(partial_logits, (1 - head) * rows, rows, 0)
    ours = lax.dynamic_slice_in_dim(partial_logits, head * rows, rows, 0)
    logits = ours + swap_heads(theirs.astype(jnp.bfloat16)).astype(jnp.float32)
    vocab_rows = logits.shape[1]
    my_index = (window * z_count + z) * cores + lax.axis_index("ctx_3")
    local_ids = lax.dynamic_slice_in_dim(ids, head * rows, rows, 0) - my_index * vocab_rows
    matches = local_ids[:, None] == jnp.arange(vocab_rows, dtype=jnp.int32)[None, :]
    target_part = jnp.sum(jnp.where(matches, logits, 0.0), axis=1)
    local_top = jnp.max(logits, axis=1)
    sum_part = jnp.sum(jnp.exp(logits - local_top[:, None]), axis=1)
    stats = jnp.stack([local_top, sum_part, target_part]).reshape(3, rows // 128, 128)
    by_z = spread(stats, ("ctx_2",))
    merged = merged_stats((by_z[:, 0], by_z[:, 1], by_z[:, 2]), 0)
    by_rest = spread(jnp.stack(merged), XYCH)
    by_rest = by_rest.reshape(-1, 2, 3, rows // 128, 128)
    top, total, target = merged_stats((by_rest[:, :, 0], by_rest[:, :, 1], by_rest[:, :, 2]), 0)
    log_probs = (target - top - jnp.log(total)).reshape(cores, row_count // (cores * count), count)
    log_probs = log_probs.swapaxes(0, 1).reshape(row_count)
    ratio = jnp.exp(jnp.clip(log_probs - old_logp, -4.0, 4.0))
    token_loss = -jnp.minimum(ratio * advantage, jnp.clip(ratio, 0.8, 1.2) * advantage)
    return (attended, log_probs, token_loss)


def solution(mesh):
    finer = Mesh(mesh.devices.reshape(4, 2, 8, 2, mesh.shape["head"]), AXES)
    ctx = AXES[:4]
    placed = (
        P(ctx, "head"),
        P(ctx, "head"),
        P(ctx, "head"),
        P(),
        P(ctx),
        P(ctx, "head"),
        P("head"),
        P("head", None),
        P("head", ctx),
        P(),
        P(),
        P(),
    )
    return jax.shard_map(
        per_device,
        mesh=finer,
        in_specs=placed,
        out_specs=(P(ctx, "head"), P(), P()),
        check_vma=False,
    )
```

```python
import functools

import jax
import jax.numpy as jnp
from jax import lax
from jax.experimental import pallas as pl
from jax.experimental.pallas import tpu as pltpu
from jax.sharding import Mesh
from jax.sharding import PartitionSpec as P

HEAD_SIZE = 128
GROUP = 4
DOCS = 8
AXES = ("ctx_0", "ctx_1", "ctx_2", "ctx_3", "head")
XYC = ("ctx_0", "ctx_1", "ctx_3")
XY = ("ctx_0", "ctx_1")
CTX = AXES[:4]
XYCH = ("ctx_0", "ctx_1", "ctx_3", "head")

LOG2E = 1.4426950408889634
SCORE_TO_LOG2 = HEAD_SIZE ** (-0.5) * LOG2E
MASKED = -1e30
NO_TOP = -1e20


def size_of(axes):
    n = 1
    for a in axes:
        n *= lax.axis_size(a)
    return n


def spread(shard, axes):
    n = size_of(axes)
    return lax.all_to_all(
        jnp.broadcast_to(shard[None], (n, *shard.shape)), axes, 0, 0, tiled=True
    )


def swap_heads(shard):
    return lax.ppermute(shard, "head", [(0, 1), (1, 0)])


def attention_kernel(meta_ref, q_ref, *refs):
    chunks = len(refs) - 6
    kv_refs = refs[:chunks]
    out_ref, k_ref, v_ref, m_ref, acc_ref, s_ref = refs[chunks:]
    j = pl.program_id(0)
    half = out_ref.shape[1]
    chunk_rows = 2 * half
    span = chunks * chunk_rows
    rows = 2 * half
    z = meta_ref[DOCS]
    window = meta_ref[DOCS + 1]
    core = meta_ref[DOCS + 2]

    @pl.when(j == 0)
    def _():
        v_ref[:, HEAD_SIZE:] = jnp.ones((span, HEAD_SIZE), jnp.bfloat16)
        for d in range(chunks):
            base = ((z - d) & (chunks - 1)) * chunk_rows
            for side in range(2):
                place = core if side == 0 else 1 - core
                at = pl.multiple_of(base + place * half, half)
                k_ref[pl.ds(at, half), :] = kv_refs[d][side, :, :HEAD_SIZE]
                v_ref[pl.ds(at, half), :HEAD_SIZE] = kv_refs[d][side, :, HEAD_SIZE:]

    first_q = j * span + z * chunk_rows
    last_q = first_q + rows - 1
    first_k = window * chunk_rows

    def start_of(pos):
        low = jnp.int32(0)
        for d in range(DOCS):
            start = meta_ref[d]
            low = jnp.where(start <= pos, jnp.maximum(low, start), low)
        return low

    low_first = start_of(first_q)
    low_last = start_of(last_q)
    m_ref[...] = jnp.full(m_ref.shape, NO_TOP, jnp.float32)
    acc_ref[...] = jnp.zeros(acc_ref.shape, jnp.float32)
    chunk_lo = jnp.maximum(low_first - first_k - chunk_rows + span, 0) // span
    chunk_hi = (last_q - first_k + span) // span

    def score(i, masked):
        at = pl.multiple_of(i * chunk_rows, chunk_rows)
        k = k_ref[pl.ds(at, chunk_rows), :]
        if masked:
            pos = first_q + lax.broadcasted_iota(jnp.int32, (rows, 1), 0)
            low = jnp.zeros((rows, 1), jnp.int32)
            for d in range(DOCS):
                start = meta_ref[d]
                low = jnp.where(start <= pos, jnp.maximum(low, start), low)
            base = first_k + i * span
            key = lax.broadcasted_iota(jnp.int32, (rows, chunk_rows), 1)
            allowed = (key >= low - base) & (key <= pos - base)
        for g in range(GROUP):
            q = q_ref[:, :, g * HEAD_SIZE : (g + 1) * HEAD_SIZE].reshape(rows, HEAD_SIZE)
            s = lax.dot_general(
                q, k, (((1,), (1,)), ((), ())), preferred_element_type=jnp.float32
            )
            if masked:
                s = jnp.where(allowed, s, MASKED)
            s_ref[g, i] = s
            top = m_ref[g]
            for h in range(chunk_rows // HEAD_SIZE):
                top = jnp.maximum(top, s[:, h * HEAD_SIZE : (h + 1) * HEAD_SIZE])
            m_ref[g] = top

    def score_step(i, carry):
        base = first_k + i * span
        free = (base >= low_last) & (base + chunk_rows - 1 <= first_q)

        @pl.when(free)
        def _():
            score(i, False)

        @pl.when(jnp.logical_not(free))
        def _():
            score(i, True)

        return carry

    lax.fori_loop(chunk_lo, chunk_hi, score_step, 0)
    for g in range(GROUP):
        top = jnp.max(m_ref[g], axis=1, keepdims=True) * SCORE_TO_LOG2
        top = jnp.maximum(top, NO_TOP).astype(jnp.bfloat16).astype(jnp.float32)
        m_ref[g] = jnp.broadcast_to(top, (rows, HEAD_SIZE))

    def weigh_step(i, carry):
        at = pl.multiple_of(i * chunk_rows, chunk_rows)
        v = v_ref[pl.ds(at, chunk_rows), :]
        for g in range(GROUP):
            top = m_ref[g]
            top = jnp.concatenate([top] * (chunk_rows // HEAD_SIZE), axis=1)
            p = jnp.exp2(s_ref[g, i] * SCORE_TO_LOG2 - top).astype(jnp.bfloat16)
            acc_ref[g] += jnp.dot(p, v, preferred_element_type=jnp.float32)
        return carry

    lax.fori_loop(chunk_lo, chunk_hi, weigh_step, 0)

    lane = lax.broadcasted_iota(jnp.int32, (rows, HEAD_SIZE), 1)
    total = jnp.zeros((rows, HEAD_SIZE), jnp.float32)
    top = jnp.zeros((rows, HEAD_SIZE), jnp.float32)
    for g in range(GROUP):
        out_ref[:, :, g * HEAD_SIZE : (g + 1) * HEAD_SIZE] = (
            acc_ref[g, :, :HEAD_SIZE].astype(jnp.bfloat16).reshape(2, half, HEAD_SIZE)
        )
        mine = lane % GROUP == g
        total = jnp.where(mine, acc_ref[g, :, HEAD_SIZE:], total)
        top = jnp.where(mine, m_ref[g], top)
    high = total.astype(jnp.bfloat16).astype(jnp.float32)
    middle = (total - high).astype(jnp.bfloat16).astype(jnp.float32)
    low = total - high - middle
    stats = jnp.where(lane < GROUP, top, high)
    stats = jnp.where(lane >= 2 * GROUP, middle, stats)
    stats = jnp.where(lane >= 3 * GROUP, low, stats)
    stats = jnp.where(lane >= 4 * GROUP, 0.0, stats)
    out_ref[:, :, GROUP * HEAD_SIZE :] = stats.astype(jnp.bfloat16).reshape(
        2, half, HEAD_SIZE
    )


def partial_attention(meta, q_all, kv_all):
    blocks, half, width = q_all.shape
    chunks = len(kv_all)
    rows = 2 * half
    keys = chunks * rows
    wide = width + HEAD_SIZE
    return pl.pallas_call(
        attention_kernel,
        grid_spec=pltpu.PrefetchScalarGridSpec(
            num_scalar_prefetch=1,
            grid=(blocks // 2,),
            in_specs=[pl.BlockSpec((2, half, width), lambda j, meta: (j, 0, 0))]
            + [pl.BlockSpec((2, half, 2 * HEAD_SIZE), lambda j, meta: (0, 0, 0))] * chunks,
            out_specs=pl.BlockSpec((2, half, wide), lambda j, meta: (j, 0, 0)),
            scratch_shapes=[
                pltpu.VMEM((keys, HEAD_SIZE), jnp.bfloat16),
                pltpu.VMEM((keys, 2 * HEAD_SIZE), jnp.bfloat16),
                pltpu.VMEM((GROUP, rows, HEAD_SIZE), jnp.float32),
                pltpu.VMEM((GROUP, rows, 2 * HEAD_SIZE), jnp.float32),
                pltpu.VMEM((GROUP, chunks, rows, rows), jnp.float32),
            ],
        ),
        out_shape=jax.ShapeDtypeStruct((blocks, half, wide), jnp.bfloat16),
        compiler_params=pltpu.CompilerParams(dimension_semantics=("arbitrary",)),
        name="partial_attention",
    )(meta, q_all, *kv_all)


def merge_kernel(scored_ref, parts_ref, attended_ref, chosen_ref):
    windows = parts_ref.shape[0] // 2
    rows = parts_ref.shape[1]
    for c in range(2):
        tops, sums = [], []
        for w in range(windows):
            st = parts_ref[2 * w + c, :, GROUP * HEAD_SIZE :].astype(jnp.float32)
            tops.append(st)
            sums.append(
                pltpu.roll(st, HEAD_SIZE - GROUP, 1)
                + pltpu.roll(st, HEAD_SIZE - 2 * GROUP, 1)
                + pltpu.roll(st, HEAD_SIZE - 3 * GROUP, 1)
            )
        top = functools.reduce(jnp.maximum, tops)
        shares = [jnp.exp2(t - top) for t in tops]
        total = functools.reduce(jnp.add, [n * share for n, share in zip(sums, shares)])
        lane = lax.broadcasted_iota(jnp.int32, total.shape, 1)
        total = jnp.where(lane < GROUP, total, 1.0)
        shares = [share / total for share in shares]
        for g in range(GROUP):
            result = jnp.zeros((rows, HEAD_SIZE), jnp.float32)
            for w in range(windows):
                part = parts_ref[2 * w + c, :, g * HEAD_SIZE : (g + 1) * HEAD_SIZE]
                result = result + shares[w][:, g : g + 1] * part.astype(jnp.float32)
            at = (c * GROUP + g) * HEAD_SIZE
            attended_ref[:, at : at + HEAD_SIZE] = result.astype(jnp.bfloat16)
    count = scored_ref.shape[0]
    row = lax.broadcasted_iota(jnp.int32, (chosen_ref.shape[0], rows), 0)
    col = lax.broadcasted_iota(jnp.int32, (chosen_ref.shape[0], rows), 1)
    pick = jnp.zeros((chosen_ref.shape[0], rows), jnp.float32)
    for i in range(count):
        pick = jnp.where((row == i) & (col == scored_ref[i]), 1.0, pick)
    chosen_ref[...] = jnp.dot(
        pick.astype(jnp.bfloat16), attended_ref[...], preferred_element_type=jnp.float32
    ).astype(jnp.bfloat16)


def merged_attention(scored, parts):
    rows = parts.shape[1]
    width = 2 * GROUP * HEAD_SIZE
    return pl.pallas_call(
        merge_kernel,
        in_specs=[
            pl.BlockSpec(memory_space=pltpu.SMEM),
            pl.BlockSpec(memory_space=pltpu.VMEM),
        ],
        out_specs=(
            pl.BlockSpec(memory_space=pltpu.VMEM),
            pl.BlockSpec(memory_space=pltpu.VMEM),
        ),
        out_shape=(
            jax.ShapeDtypeStruct((rows, width), jnp.bfloat16),
            jax.ShapeDtypeStruct((16, width), jnp.bfloat16),
        ),
        name="merged_attention",
    )(scored, parts)


def merged_stats(stats, axis):
    tops, sums, targets = stats
    top = jnp.max(tops, axis=axis)
    total = jnp.sum(sums * jnp.exp(tops - jnp.expand_dims(top, axis)), axis=axis)
    return (top, total, jnp.sum(targets, axis=axis))


def per_device(
    queries,
    rotated_keys,
    value_matrix,
    doc_lengths,
    scored,
    residual,
    norm_gain,
    out_weight,
    lm_weight,
    token_ids,
    old_logp,
    advantage,
):
    tok_rows = queries.shape[0]
    count = scored.shape[0]
    cores = lax.axis_size("ctx_3")
    window_count = size_of(XY)
    z_count = lax.axis_size("ctx_2")
    window = lax.axis_index(XY)
    z = lax.axis_index("ctx_2")

    doc_starts = jnp.cumsum(doc_lengths) - doc_lengths
    core = lax.axis_index("ctx_3")
    meta = jnp.concatenate(
        [doc_starts.astype(jnp.int32), jnp.stack([z, window, core]).astype(jnp.int32)]
    )

    def of_head(c):
        at = c * HEAD_SIZE
        return jnp.concatenate(
            [
                lax.dynamic_slice_in_dim(rotated_keys, at, HEAD_SIZE, 1),
                lax.dynamic_slice_in_dim(value_matrix, at, HEAD_SIZE, 1),
            ],
            axis=1,
        )

    same, cross = [], []
    for w in range(window_count):
        for k in range(z_count):
            for c in range(cores):
                here, there = (w * z_count + k) * cores, (k * z_count + w) * cores
                same.append((here + c, there + c))
                cross.append((here + c, there + 1 - c))
    own_chunk = jnp.stack(
        [
            lax.ppermute(of_head(core), CTX, same),
            lax.ppermute(of_head(1 - core), CTX, cross),
        ]
    )
    kv_all = [own_chunk] + [
        lax.ppermute(own_chunk, "ctx_2", [(k, (k + d) % z_count) for k in range(z_count)])
        for d in range(1, z_count)
    ]
    by_core = jnp.swapaxes(queries.reshape(tok_rows, cores, GROUP * HEAD_SIZE), 0, 1)
    q_send = jnp.broadcast_to(by_core[None], (window_count, *by_core.shape)).reshape(
        window_count * cores, tok_rows, GROUP * HEAD_SIZE
    )
    q_all = lax.all_to_all(q_send, XYC, 0, 0, tiled=True)
    parts = partial_attention(meta, q_all, kv_all)
    arrived = lax.all_to_all(parts, XYC, 0, 0, tiled=True)
    attended, chosen = merged_attention(scored, arrived)

    half = residual.shape[1]
    head = lax.axis_index("head")
    partial_value = jnp.dot(chosen, out_weight, preferred_element_type=jnp.float32)[:count]
    own = lax.dynamic_slice_in_dim(partial_value, head * half, half, 1)
    own = own + residual.astype(jnp.float32)
    partial_value = lax.dynamic_update_slice_in_dim(partial_value, own, head * half, 1)
    other = swap_heads(partial_value.astype(jnp.bfloat16)).astype(jnp.float32)
    hidden_all = partial_value + other
    squares = jnp.sum(hidden_all * hidden_all, axis=1, keepdims=True)
    hidden = own + lax.dynamic_slice_in_dim(other, head * half, half, 1)
    normed = (
        hidden * lax.rsqrt(squares / hidden_all.shape[1] + 1e-05) * norm_gain[None, :]
    ).astype(jnp.bfloat16)

    along_z = spread(normed, ("ctx_2",))
    along_xy = spread(along_z, XY)
    everyone = spread(along_xy, ("ctx_3",)).reshape(-1, half)
    row_count = everyone.shape[0]
    ids = token_ids.reshape(-1, cores, count).swapaxes(0, 1).reshape(row_count)
    partial_logits = jnp.dot(everyone, lm_weight, preferred_element_type=jnp.float32)
    rows = row_count // 2
    theirs = lax.dynamic_slice_in_dim(partial_logits, (1 - head) * rows, rows, 0)
    ours = lax.dynamic_slice_in_dim(partial_logits, head * rows, rows, 0)
    logits = ours + swap_heads(theirs.astype(jnp.bfloat16)).astype(jnp.float32)
    vocab_rows = logits.shape[1]
    my_index = (window * z_count + z) * cores + core
    local_ids = lax.dynamic_slice_in_dim(ids, head * rows, rows, 0) - my_index * vocab_rows
    matches = local_ids[:, None] == jnp.arange(vocab_rows, dtype=jnp.int32)[None, :]
    target_part = jnp.sum(jnp.where(matches, logits, 0.0), axis=1)
    local_top = jnp.max(logits, axis=1)
    sum_part = jnp.sum(jnp.exp(logits - local_top[:, None]), axis=1)
    stats = jnp.stack([local_top, sum_part, target_part]).reshape(3, rows // 128, 128)
    by_z = spread(stats, ("ctx_2",))
    merged = merged_stats((by_z[:, 0], by_z[:, 1], by_z[:, 2]), 0)
    by_rest = spread(jnp.stack(merged), XYCH)
    by_rest = by_rest.reshape(-1, 2, 3, rows // 128, 128)
    top, total, target = merged_stats((by_rest[:, :, 0], by_rest[:, :, 1], by_rest[:, :, 2]), 0)
    log_probs = (target - top - jnp.log(total)).reshape(cores, row_count // (cores * count), count)
    log_probs = log_probs.swapaxes(0, 1).reshape(row_count)
    ratio = jnp.exp(jnp.clip(log_probs - old_logp, -4.0, 4.0))
    token_loss = -jnp.minimum(ratio * advantage, jnp.clip(ratio, 0.8, 1.2) * advantage)
    return (attended, log_probs, token_loss)


def solution(mesh):
    finer = Mesh(mesh.devices.reshape(4, 2, 8, 2, mesh.shape["head"]), AXES)
    ctx = AXES[:4]
    placed = (
        P(ctx, "head"),
        P(ctx, "head"),
        P(ctx, "head"),
        P(),
        P(ctx),
        P(ctx, "head"),
        P("head"),
        P("head", None),
        P("head", ctx),
        P(),
        P(),
        P(),
    )
    return jax.shard_map(
        per_device,
        mesh=finer,
        in_specs=placed,
        out_specs=(P(ctx, "head"), P(), P()),
        check_vma=False,
    )
```

```python
import functools

import jax
import jax.numpy as jnp
from jax import lax
from jax.experimental import pallas as pl
from jax.experimental.pallas import tpu as pltpu
from jax.sharding import Mesh
from jax.sharding import PartitionSpec as P

HEAD_SIZE = 128
GROUP = 4
DOCS = 8
AXES = ("ctx_0", "ctx_1", "ctx_2", "ctx_3", "head")
CTX = AXES[:4]
XC = ("ctx_0", "ctx_3")
YZ = ("ctx_1", "ctx_2")
XYCH = ("ctx_0", "ctx_1", "ctx_3", "head")

LOG2E = 1.4426950408889634
SCORE_TO_LOG2 = HEAD_SIZE ** (-0.5) * LOG2E
MASKED = -1e30
NO_TOP = -1e20


def size_of(axes):
    n = 1
    for a in axes:
        n *= lax.axis_size(a)
    return n


def spread(shard, axes):
    n = size_of(axes)
    return lax.all_to_all(
        jnp.broadcast_to(shard[None], (n, *shard.shape)), axes, 0, 0, tiled=True
    )


def swap_heads(shard):
    return lax.ppermute(shard, "head", [(0, 1), (1, 0)])


def attention_kernel(meta_ref, q_ref, *refs):
    groups = len(refs) - 6
    kv_refs = refs[:groups]
    out_ref, k_ref, v_ref, m_ref, acc_ref, s_ref = refs[groups:]
    j = pl.program_id(0)
    half = out_ref.shape[1]
    rows = 2 * half
    chunk_rows = s_ref.shape[3]
    chunks = s_ref.shape[1]
    x, y, z, core = [meta_ref[DOCS + n] for n in range(4)]
    span = groups * rows

    @pl.when(j == 0)
    def _():
        v_ref[:, HEAD_SIZE:] = jnp.ones((chunks * chunk_rows, HEAD_SIZE), jnp.bfloat16)
        for d in range(groups):
            place = (z - d) & (groups - 1)
            for dy in range(2):
                base = ((place // 2) * 2 + (y ^ dy)) * chunk_rows + (place & 1) * rows
                for dc in range(2):
                    at = pl.multiple_of(base + (core ^ dc) * half, half)
                    k_ref[pl.ds(at, half), :] = kv_refs[d][dy, dc, :, :HEAD_SIZE]
                    v_ref[pl.ds(at, half), :HEAD_SIZE] = kv_refs[d][dy, dc, :, HEAD_SIZE:]

    first_q = (2 * j + y) * span + z * rows
    last_q = first_q + rows - 1
    first_k = x * chunk_rows

    def start_of(pos):
        low = jnp.int32(0)
        for d in range(DOCS):
            start = meta_ref[d]
            low = jnp.where(start <= pos, jnp.maximum(low, start), low)
        return low

    low_first = start_of(first_q)
    low_last = start_of(last_q)
    m_ref[...] = jnp.full(m_ref.shape, NO_TOP, jnp.float32)
    acc_ref[...] = jnp.zeros(acc_ref.shape, jnp.float32)
    chunk_lo = jnp.maximum(low_first - first_k - chunk_rows + span, 0) // span
    chunk_hi = (last_q - first_k + span) // span

    def score(i, masked):
        at = pl.multiple_of(i * chunk_rows, chunk_rows)
        k = k_ref[pl.ds(at, chunk_rows), :]
        if masked:
            pos = first_q + lax.broadcasted_iota(jnp.int32, (rows, 1), 0)
            low = jnp.zeros((rows, 1), jnp.int32)
            for d in range(DOCS):
                start = meta_ref[d]
                low = jnp.where(start <= pos, jnp.maximum(low, start), low)
            base = first_k + i * span
            key = lax.broadcasted_iota(jnp.int32, (rows, chunk_rows), 1)
            allowed = (key >= low - base) & (key <= pos - base)
        for g in range(GROUP):
            q = q_ref[:, :, g * HEAD_SIZE : (g + 1) * HEAD_SIZE].reshape(rows, HEAD_SIZE)
            s = lax.dot_general(
                q, k, (((1,), (1,)), ((), ())), preferred_element_type=jnp.float32
            )
            if masked:
                s = jnp.where(allowed, s, MASKED)
            s_ref[g, i] = s
            top = m_ref[g]
            for h in range(chunk_rows // HEAD_SIZE):
                top = jnp.maximum(top, s[:, h * HEAD_SIZE : (h + 1) * HEAD_SIZE])
            m_ref[g] = top

    def score_step(i, carry):
        base = first_k + i * span
        free = (base >= low_last) & (base + chunk_rows - 1 <= first_q)

        @pl.when(free)
        def _():
            score(i, False)

        @pl.when(jnp.logical_not(free))
        def _():
            score(i, True)

        return carry

    lax.fori_loop(chunk_lo, chunk_hi, score_step, 0)
    for g in range(GROUP):
        top = jnp.max(m_ref[g], axis=1, keepdims=True) * SCORE_TO_LOG2
        top = jnp.maximum(top, NO_TOP).astype(jnp.bfloat16).astype(jnp.float32)
        m_ref[g] = jnp.broadcast_to(top, (rows, HEAD_SIZE))

    def weigh_step(i, carry):
        at = pl.multiple_of(i * chunk_rows, chunk_rows)
        v = v_ref[pl.ds(at, chunk_rows), :]
        for g in range(GROUP):
            top = m_ref[g]
            top = jnp.concatenate([top] * (chunk_rows // HEAD_SIZE), axis=1)
            p = jnp.exp2(s_ref[g, i] * SCORE_TO_LOG2 - top).astype(jnp.bfloat16)
            acc_ref[g] += jnp.dot(p, v, preferred_element_type=jnp.float32)
        return carry

    lax.fori_loop(chunk_lo, chunk_hi, weigh_step, 0)

    lane = lax.broadcasted_iota(jnp.int32, (rows, HEAD_SIZE), 1)
    total = jnp.zeros((rows, HEAD_SIZE), jnp.float32)
    top = jnp.zeros((rows, HEAD_SIZE), jnp.float32)
    for g in range(GROUP):
        out_ref[:, :, g * HEAD_SIZE : (g + 1) * HEAD_SIZE] = (
            acc_ref[g, :, :HEAD_SIZE].astype(jnp.bfloat16).reshape(2, half, HEAD_SIZE)
        )
        mine = lane % GROUP == g
        total = jnp.where(mine, acc_ref[g, :, HEAD_SIZE:], total)
        top = jnp.where(mine, m_ref[g], top)
    high = total.astype(jnp.bfloat16).astype(jnp.float32)
    middle = (total - high).astype(jnp.bfloat16).astype(jnp.float32)
    low = total - high - middle
    stats = jnp.where(lane < GROUP, top, high)
    stats = jnp.where(lane >= 2 * GROUP, middle, stats)
    stats = jnp.where(lane >= 3 * GROUP, low, stats)
    stats = jnp.where(lane >= 4 * GROUP, 0.0, stats)
    out_ref[:, :, GROUP * HEAD_SIZE :] = stats.astype(jnp.bfloat16).reshape(
        2, half, HEAD_SIZE
    )


def partial_attention(meta, q_all, kv_all):
    blocks, half, width = q_all.shape
    rows = 2 * half
    keys = 2 * rows * len(kv_all)
    chunk_rows = 2 * rows
    wide = width + HEAD_SIZE
    return pl.pallas_call(
        attention_kernel,
        grid_spec=pltpu.PrefetchScalarGridSpec(
            num_scalar_prefetch=1,
            grid=(blocks // 2,),
            in_specs=[pl.BlockSpec((2, half, width), lambda j, meta: (j, 0, 0))]
            + [pl.BlockSpec((2, 2, half, 2 * HEAD_SIZE), lambda j, meta: (0, 0, 0, 0))]
            * len(kv_all),
            out_specs=pl.BlockSpec((2, half, wide), lambda j, meta: (j, 0, 0)),
            scratch_shapes=[
                pltpu.VMEM((keys, HEAD_SIZE), jnp.bfloat16),
                pltpu.VMEM((keys, 2 * HEAD_SIZE), jnp.bfloat16),
                pltpu.VMEM((GROUP, rows, HEAD_SIZE), jnp.float32),
                pltpu.VMEM((GROUP, rows, 2 * HEAD_SIZE), jnp.float32),
                pltpu.VMEM((GROUP, keys // chunk_rows, rows, chunk_rows), jnp.float32),
            ],
        ),
        out_shape=jax.ShapeDtypeStruct((blocks, half, wide), jnp.bfloat16),
        compiler_params=pltpu.CompilerParams(dimension_semantics=("arbitrary",)),
        name="partial_attention",
    )(meta, q_all, *kv_all)


def merge_kernel(scored_ref, parts_ref, attended_ref, chosen_ref):
    windows = parts_ref.shape[0] // 2
    rows = parts_ref.shape[1]
    for c in range(2):
        tops, sums = [], []
        for w in range(windows):
            st = parts_ref[2 * w + c, :, GROUP * HEAD_SIZE :].astype(jnp.float32)
            tops.append(st)
            sums.append(
                pltpu.roll(st, HEAD_SIZE - GROUP, 1)
                + pltpu.roll(st, HEAD_SIZE - 2 * GROUP, 1)
                + pltpu.roll(st, HEAD_SIZE - 3 * GROUP, 1)
            )
        top = functools.reduce(jnp.maximum, tops)
        shares = [jnp.exp2(t - top) for t in tops]
        total = functools.reduce(jnp.add, [n * share for n, share in zip(sums, shares)])
        lane = lax.broadcasted_iota(jnp.int32, total.shape, 1)
        total = jnp.where(lane < GROUP, total, 1.0)
        shares = [share / total for share in shares]
        for g in range(GROUP):
            result = jnp.zeros((rows, HEAD_SIZE), jnp.float32)
            for w in range(windows):
                part = parts_ref[2 * w + c, :, g * HEAD_SIZE : (g + 1) * HEAD_SIZE]
                result = result + shares[w][:, g : g + 1] * part.astype(jnp.float32)
            at = (c * GROUP + g) * HEAD_SIZE
            attended_ref[:, at : at + HEAD_SIZE] = result.astype(jnp.bfloat16)
    count = scored_ref.shape[0]
    row = lax.broadcasted_iota(jnp.int32, (chosen_ref.shape[0], rows), 0)
    col = lax.broadcasted_iota(jnp.int32, (chosen_ref.shape[0], rows), 1)
    pick = jnp.zeros((chosen_ref.shape[0], rows), jnp.float32)
    for i in range(count):
        pick = jnp.where((row == i) & (col == scored_ref[i]), 1.0, pick)
    chosen_ref[...] = jnp.dot(
        pick.astype(jnp.bfloat16), attended_ref[...], preferred_element_type=jnp.float32
    ).astype(jnp.bfloat16)


def merged_attention(scored, parts):
    rows = parts.shape[1]
    width = 2 * GROUP * HEAD_SIZE
    return pl.pallas_call(
        merge_kernel,
        in_specs=[
            pl.BlockSpec(memory_space=pltpu.SMEM),
            pl.BlockSpec(memory_space=pltpu.VMEM),
        ],
        out_specs=(
            pl.BlockSpec(memory_space=pltpu.VMEM),
            pl.BlockSpec(memory_space=pltpu.VMEM),
        ),
        out_shape=(
            jax.ShapeDtypeStruct((rows, width), jnp.bfloat16),
            jax.ShapeDtypeStruct((16, width), jnp.bfloat16),
        ),
        name="merged_attention",
    )(scored, parts)


def merged_stats(stats, axis):
    tops, sums, targets = stats
    top = jnp.max(tops, axis=axis)
    total = jnp.sum(sums * jnp.exp(tops - jnp.expand_dims(top, axis)), axis=axis)
    return (top, total, jnp.sum(targets, axis=axis))


def per_device(
    queries,
    rotated_keys,
    value_matrix,
    doc_lengths,
    scored,
    residual,
    norm_gain,
    out_weight,
    lm_weight,
    token_ids,
    old_logp,
    advantage,
):
    tok_rows = queries.shape[0]
    count = scored.shape[0]
    nx, ny, nz, cores = [lax.axis_size(a) for a in CTX]
    x, y, z, core = [lax.axis_index(a) for a in CTX]
    doc_starts = jnp.cumsum(doc_lengths) - doc_lengths
    meta = jnp.concatenate(
        [doc_starts.astype(jnp.int32), jnp.stack([x, y, z, core]).astype(jnp.int32)]
    )

    def of_head(c):
        at = c * HEAD_SIZE
        return jnp.concatenate(
            [
                lax.dynamic_slice_in_dim(rotated_keys, at, HEAD_SIZE, 1),
                lax.dynamic_slice_in_dim(value_matrix, at, HEAD_SIZE, 1),
            ],
            axis=1,
        )

    def handed(dy, dc):
        return [
            (
                ((i * ny + k) * nz + high * 2 + low) * cores + c,
                ((high * ny + (k ^ dy)) * nz + i * 2 + low) * cores + (c ^ dc),
            )
            for i in range(nx)
            for k in range(ny)
            for high in range(nz // 2)
            for low in range(2)
            for c in range(cores)
        ]

    mine, others = of_head(core), of_head(1 - core)
    own = jnp.stack(
        [
            jnp.stack([lax.ppermute(mine, CTX, handed(dy, 0)), lax.ppermute(others, CTX, handed(dy, 1))])
            for dy in range(ny)
        ]
    )

    def shifted(a, d):
        return lax.ppermute(a, "ctx_2", [(k, (k + d) % nz) for k in range(nz)])

    kv_all = [own] + [None] * (nz - 1)
    for d in range(1, nz // 2):
        kv_all[d] = shifted(kv_all[d - 1], 1)
        kv_all[nz - d] = shifted(kv_all[(nz - d + 1) % nz], -1)
    far = nz // 2
    kv_all[far] = jnp.stack([shifted(kv_all[far - 1][0], 1), shifted(kv_all[far + 1][1], -1)])

    by_core = jnp.swapaxes(queries.reshape(tok_rows, cores, GROUP * HEAD_SIZE), 0, 1)
    q_send = jnp.broadcast_to(by_core[None], (nx, *by_core.shape)).reshape(
        nx * cores, tok_rows, GROUP * HEAD_SIZE
    )
    q_all = lax.all_to_all(q_send, XC, 0, 0, tiled=True)
    parts = partial_attention(meta, q_all, kv_all)
    arrived = lax.all_to_all(parts, XC, 0, 0, tiled=True)
    attended, chosen = merged_attention(scored, arrived)

    half = residual.shape[1]
    head = lax.axis_index("head")
    partial_value = jnp.dot(chosen, out_weight, preferred_element_type=jnp.float32)[:count]
    own = lax.dynamic_slice_in_dim(partial_value, head * half, half, 1)
    own = own + residual.astype(jnp.float32)
    partial_value = lax.dynamic_update_slice_in_dim(partial_value, own, head * half, 1)
    other = swap_heads(partial_value.astype(jnp.bfloat16)).astype(jnp.float32)
    hidden_all = partial_value + other
    squares = jnp.sum(hidden_all * hidden_all, axis=1, keepdims=True)
    hidden = own + lax.dynamic_slice_in_dim(other, head * half, half, 1)
    normed = (
        hidden * lax.rsqrt(squares / hidden_all.shape[1] + 1e-05) * norm_gain[None, :]
    ).astype(jnp.bfloat16)

    own_rows = spread(spread(normed, YZ), ("ctx_0",)).reshape(-1, half)
    other_rows = lax.ppermute(own_rows, "ctx_3", [(0, 1), (1, 0)])
    rows = own_rows.shape[0] // 2
    chips = nx * ny * nz
    vocab_rows = lm_weight.shape[1]
    my_index = ((x * ny + y) * nz + z) * cores + core
    ids = token_ids.reshape(chips, cores, count).swapaxes(0, 1).reshape(cores, 2, rows)
    ids = lax.dynamic_index_in_dim(ids, head, 1, keepdims=False) - my_index * vocab_rows

    def local_stats(normed_rows, local_ids):
        partial_logits = jnp.dot(normed_rows, lm_weight, preferred_element_type=jnp.float32)
        theirs = lax.dynamic_slice_in_dim(partial_logits, (1 - head) * rows, rows, 0)
        ours = lax.dynamic_slice_in_dim(partial_logits, head * rows, rows, 0)
        logits = ours + swap_heads(theirs.astype(jnp.bfloat16)).astype(jnp.float32)
        matches = local_ids[:, None] == jnp.arange(vocab_rows, dtype=jnp.int32)[None, :]
        target_part = jnp.sum(jnp.where(matches, logits, 0.0), axis=1)
        local_top = jnp.max(logits, axis=1)
        sum_part = jnp.sum(jnp.exp(logits - local_top[:, None]), axis=1)
        return jnp.stack([local_top, sum_part, target_part])

    ids_first = lax.dynamic_index_in_dim(ids, core, 0, keepdims=False)
    ids_second = lax.dynamic_index_in_dim(ids, 1 - core, 0, keepdims=False)
    first = local_stats(own_rows, ids_first)
    second = local_stats(other_rows, ids_second)
    stats = jnp.where(core == 0, jnp.stack([first, second]), jnp.stack([second, first]))
    by_z = spread(stats, ("ctx_2",))
    merged = merged_stats((by_z[:, :, 0], by_z[:, :, 1], by_z[:, :, 2]), 0)
    by_rest = spread(jnp.stack(merged), XYCH)
    by_rest = by_rest.reshape(-1, 2, 3, cores, rows)
    top, total, target = merged_stats((by_rest[:, :, 0], by_rest[:, :, 1], by_rest[:, :, 2]), 0)
    log_probs = (target - top - jnp.log(total)).reshape(2, cores, rows // count, count)
    log_probs = log_probs.swapaxes(1, 2).reshape(chips * cores * count)
    ratio = jnp.exp(jnp.clip(log_probs - old_logp, -4.0, 4.0))
    token_loss = -jnp.minimum(ratio * advantage, jnp.clip(ratio, 0.8, 1.2) * advantage)
    return (attended, log_probs, token_loss)


def solution(mesh):
    finer = Mesh(mesh.devices.reshape(4, 2, 8, 2, mesh.shape["head"]), AXES)
    ctx = AXES[:4]
    placed = (
        P(ctx, "head"),
        P(ctx, "head"),
        P(ctx, "head"),
        P(),
        P(ctx),
        P(ctx, "head"),
        P("head"),
        P("head", None),
        P("head", ctx),
        P(),
        P(),
        P(),
    )
    return jax.shard_map(
        per_device,
        mesh=finer,
        in_specs=placed,
        out_specs=(P(ctx, "head"), P(), P()),
        check_vma=False,
    )
```

```python
import functools

import jax
import jax.numpy as jnp
from jax import lax
from jax.experimental import pallas as pl
from jax.experimental.pallas import tpu as pltpu
from jax.sharding import Mesh
from jax.sharding import PartitionSpec as P

HEAD_SIZE = 128
GROUP = 4
DOCS = 8
AXES = ("ctx_0", "ctx_1", "ctx_2", "ctx_3", "head")
CTX = AXES[:4]
XC = ("ctx_0", "ctx_3")
YZ = ("ctx_1", "ctx_2")
XYCH = ("ctx_0", "ctx_1", "ctx_3", "head")

LOG2E = 1.4426950408889634
SCORE_TO_LOG2 = HEAD_SIZE ** (-0.5) * LOG2E
MASKED = -1e30
NO_TOP = -1e20


def size_of(axes):
    n = 1
    for a in axes:
        n *= lax.axis_size(a)
    return n


def spread(shard, axes):
    n = size_of(axes)
    return lax.all_to_all(
        jnp.broadcast_to(shard[None], (n, *shard.shape)), axes, 0, 0, tiled=True
    )


def swap_heads(shard):
    return lax.ppermute(shard, "head", [(0, 1), (1, 0)])


def attention_kernel(meta_ref, q_ref, *refs):
    groups = len(refs) - 6
    kv_refs = refs[:groups]
    out_ref, k_ref, v_ref, m_ref, acc_ref, s_ref = refs[groups:]
    j = pl.program_id(0)
    half = out_ref.shape[1]
    rows = 2 * half
    chunk_rows = s_ref.shape[3]
    chunks = s_ref.shape[1]
    x, y, z, core = [meta_ref[DOCS + n] for n in range(4)]
    span = groups * rows

    @pl.when(j == 0)
    def _():
        v_ref[:, HEAD_SIZE:] = jnp.ones((chunks * chunk_rows, HEAD_SIZE), jnp.bfloat16)
        for d in range(groups):
            place = (z - d) & (groups - 1)
            source = (x - place) & (groups // 2 - 1)
            for dy in range(2):
                base = (source * 2 + (y ^ dy)) * chunk_rows + (place // (groups // 2)) * rows
                for dc in range(2):
                    at = pl.multiple_of(base + (core ^ dc) * half, half)
                    k_ref[pl.ds(at, half), :] = kv_refs[d][dy, dc, :, :HEAD_SIZE]
                    v_ref[pl.ds(at, half), :HEAD_SIZE] = kv_refs[d][dy, dc, :, HEAD_SIZE:]

    first_q = (2 * j + y) * span + z * rows
    last_q = first_q + rows - 1
    far = span // 2
    reach = far + rows - 1

    def chunk_base(i):
        return i * span + ((x - i // 2) & (groups // 2 - 1)) * rows

    def start_of(pos):
        low = jnp.int32(0)
        for d in range(DOCS):
            start = meta_ref[d]
            low = jnp.where(start <= pos, jnp.maximum(low, start), low)
        return low

    low_first = start_of(first_q)
    low_last = start_of(last_q)
    m_ref[...] = jnp.full(m_ref.shape, NO_TOP, jnp.float32)
    acc_ref[...] = jnp.zeros(acc_ref.shape, jnp.float32)
    chunk_lo, chunk_hi = jnp.int32(0), jnp.int32(0)
    for i in range(chunks):
        base = chunk_base(i)
        chunk_lo += (base + reach < low_first).astype(jnp.int32)
        chunk_hi += (base <= last_q).astype(jnp.int32)

    def score(i, masked):
        at = pl.multiple_of(i * chunk_rows, chunk_rows)
        k = k_ref[pl.ds(at, chunk_rows), :]
        if masked:
            pos = first_q + lax.broadcasted_iota(jnp.int32, (rows, 1), 0)
            low = jnp.zeros((rows, 1), jnp.int32)
            for d in range(DOCS):
                start = meta_ref[d]
                low = jnp.where(start <= pos, jnp.maximum(low, start), low)
            base = chunk_base(i)
            key = lax.broadcasted_iota(jnp.int32, (rows, chunk_rows), 1)
            key = key + jnp.where(key >= rows, far - rows, 0)
            allowed = (key >= low - base) & (key <= pos - base)
        for g in range(GROUP):
            q = q_ref[:, :, g * HEAD_SIZE : (g + 1) * HEAD_SIZE].reshape(rows, HEAD_SIZE)
            s = lax.dot_general(
                q, k, (((1,), (1,)), ((), ())), preferred_element_type=jnp.float32
            )
            if masked:
                s = jnp.where(allowed, s, MASKED)
            s_ref[g, i] = s
            top = m_ref[g]
            for h in range(chunk_rows // HEAD_SIZE):
                top = jnp.maximum(top, s[:, h * HEAD_SIZE : (h + 1) * HEAD_SIZE])
            m_ref[g] = top

    def score_step(i, carry):
        base = chunk_base(i)
        free = (base >= low_last) & (base + reach <= first_q)

        @pl.when(free)
        def _():
            score(i, False)

        @pl.when(jnp.logical_not(free))
        def _():
            score(i, True)

        return carry

    lax.fori_loop(chunk_lo, chunk_hi, score_step, 0)
    for g in range(GROUP):
        top = jnp.max(m_ref[g], axis=1, keepdims=True) * SCORE_TO_LOG2
        top = jnp.maximum(top, NO_TOP).astype(jnp.bfloat16).astype(jnp.float32)
        m_ref[g] = jnp.broadcast_to(top, (rows, HEAD_SIZE))

    def weigh_step(i, carry):
        at = pl.multiple_of(i * chunk_rows, chunk_rows)
        v = v_ref[pl.ds(at, chunk_rows), :]
        for g in range(GROUP):
            top = m_ref[g]
            top = jnp.concatenate([top] * (chunk_rows // HEAD_SIZE), axis=1)
            p = jnp.exp2(s_ref[g, i] * SCORE_TO_LOG2 - top).astype(jnp.bfloat16)
            acc_ref[g] += jnp.dot(p, v, preferred_element_type=jnp.float32)
        return carry

    lax.fori_loop(chunk_lo, chunk_hi, weigh_step, 0)

    lane = lax.broadcasted_iota(jnp.int32, (rows, HEAD_SIZE), 1)
    total = jnp.zeros((rows, HEAD_SIZE), jnp.float32)
    top = jnp.zeros((rows, HEAD_SIZE), jnp.float32)
    for g in range(GROUP):
        out_ref[:, :, g * HEAD_SIZE : (g + 1) * HEAD_SIZE] = (
            acc_ref[g, :, :HEAD_SIZE].astype(jnp.bfloat16).reshape(2, half, HEAD_SIZE)
        )
        mine = lane % GROUP == g
        total = jnp.where(mine, acc_ref[g, :, HEAD_SIZE:], total)
        top = jnp.where(mine, m_ref[g], top)
    high = total.astype(jnp.bfloat16).astype(jnp.float32)
    middle = (total - high).astype(jnp.bfloat16).astype(jnp.float32)
    low = total - high - middle
    stats = jnp.where(lane < GROUP, top, high)
    stats = jnp.where(lane >= 2 * GROUP, middle, stats)
    stats = jnp.where(lane >= 3 * GROUP, low, stats)
    stats = jnp.where(lane >= 4 * GROUP, 0.0, stats)
    out_ref[:, :, GROUP * HEAD_SIZE :] = stats.astype(jnp.bfloat16).reshape(
        2, half, HEAD_SIZE
    )


def partial_attention(meta, q_all, kv_all):
    blocks, half, width = q_all.shape
    rows = 2 * half
    keys = 2 * rows * len(kv_all)
    chunk_rows = 2 * rows
    wide = width + HEAD_SIZE
    return pl.pallas_call(
        attention_kernel,
        grid_spec=pltpu.PrefetchScalarGridSpec(
            num_scalar_prefetch=1,
            grid=(blocks // 2,),
            in_specs=[pl.BlockSpec((2, half, width), lambda j, meta: (j, 0, 0))]
            + [pl.BlockSpec((2, 2, half, 2 * HEAD_SIZE), lambda j, meta: (0, 0, 0, 0))]
            * len(kv_all),
            out_specs=pl.BlockSpec((2, half, wide), lambda j, meta: (j, 0, 0)),
            scratch_shapes=[
                pltpu.VMEM((keys, HEAD_SIZE), jnp.bfloat16),
                pltpu.VMEM((keys, 2 * HEAD_SIZE), jnp.bfloat16),
                pltpu.VMEM((GROUP, rows, HEAD_SIZE), jnp.float32),
                pltpu.VMEM((GROUP, rows, 2 * HEAD_SIZE), jnp.float32),
                pltpu.VMEM((GROUP, keys // chunk_rows, rows, chunk_rows), jnp.float32),
            ],
        ),
        out_shape=jax.ShapeDtypeStruct((blocks, half, wide), jnp.bfloat16),
        compiler_params=pltpu.CompilerParams(dimension_semantics=("arbitrary",)),
        name="partial_attention",
    )(meta, q_all, *kv_all)


def merge_kernel(scored_ref, parts_ref, attended_ref, chosen_ref):
    windows = parts_ref.shape[0] // 2
    rows = parts_ref.shape[1]
    for c in range(2):
        tops, sums = [], []
        for w in range(windows):
            st = parts_ref[2 * w + c, :, GROUP * HEAD_SIZE :].astype(jnp.float32)
            tops.append(st)
            sums.append(
                pltpu.roll(st, HEAD_SIZE - GROUP, 1)
                + pltpu.roll(st, HEAD_SIZE - 2 * GROUP, 1)
                + pltpu.roll(st, HEAD_SIZE - 3 * GROUP, 1)
            )
        top = functools.reduce(jnp.maximum, tops)
        shares = [jnp.exp2(t - top) for t in tops]
        total = functools.reduce(jnp.add, [n * share for n, share in zip(sums, shares)])
        lane = lax.broadcasted_iota(jnp.int32, total.shape, 1)
        total = jnp.where(lane < GROUP, total, 1.0)
        shares = [share / total for share in shares]
        for g in range(GROUP):
            result = jnp.zeros((rows, HEAD_SIZE), jnp.float32)
            for w in range(windows):
                part = parts_ref[2 * w + c, :, g * HEAD_SIZE : (g + 1) * HEAD_SIZE]
                result = result + shares[w][:, g : g + 1] * part.astype(jnp.float32)
            at = (c * GROUP + g) * HEAD_SIZE
            attended_ref[:, at : at + HEAD_SIZE] = result.astype(jnp.bfloat16)
    count = scored_ref.shape[0]
    row = lax.broadcasted_iota(jnp.int32, (chosen_ref.shape[0], rows), 0)
    col = lax.broadcasted_iota(jnp.int32, (chosen_ref.shape[0], rows), 1)
    pick = jnp.zeros((chosen_ref.shape[0], rows), jnp.float32)
    for i in range(count):
        pick = jnp.where((row == i) & (col == scored_ref[i]), 1.0, pick)
    chosen_ref[...] = jnp.dot(
        pick.astype(jnp.bfloat16), attended_ref[...], preferred_element_type=jnp.float32
    ).astype(jnp.bfloat16)


def merged_attention(scored, parts):
    rows = parts.shape[1]
    width = 2 * GROUP * HEAD_SIZE
    return pl.pallas_call(
        merge_kernel,
        in_specs=[
            pl.BlockSpec(memory_space=pltpu.SMEM),
            pl.BlockSpec(memory_space=pltpu.VMEM),
        ],
        out_specs=(
            pl.BlockSpec(memory_space=pltpu.VMEM),
            pl.BlockSpec(memory_space=pltpu.VMEM),
        ),
        out_shape=(
            jax.ShapeDtypeStruct((rows, width), jnp.bfloat16),
            jax.ShapeDtypeStruct((16, width), jnp.bfloat16),
        ),
        name="merged_attention",
    )(scored, parts)


def merged_stats(stats, axis):
    tops, sums, targets = stats
    top = jnp.max(tops, axis=axis)
    total = jnp.sum(sums * jnp.exp(tops - jnp.expand_dims(top, axis)), axis=axis)
    return (top, total, jnp.sum(targets, axis=axis))


def per_device(
    queries,
    rotated_keys,
    value_matrix,
    doc_lengths,
    scored,
    residual,
    norm_gain,
    out_weight,
    lm_weight,
    token_ids,
    old_logp,
    advantage,
):
    tok_rows = queries.shape[0]
    count = scored.shape[0]
    nx, ny, nz, cores = [lax.axis_size(a) for a in CTX]
    x, y, z, core = [lax.axis_index(a) for a in CTX]
    doc_starts = jnp.cumsum(doc_lengths) - doc_lengths
    meta = jnp.concatenate(
        [doc_starts.astype(jnp.int32), jnp.stack([x, y, z, core]).astype(jnp.int32)]
    )

    def of_head(c):
        at = c * HEAD_SIZE
        return jnp.concatenate(
            [
                lax.dynamic_slice_in_dim(rotated_keys, at, HEAD_SIZE, 1),
                lax.dynamic_slice_in_dim(value_matrix, at, HEAD_SIZE, 1),
            ],
            axis=1,
        )

    def handed(dy, dc):
        return [
            (
                ((i * ny + k) * nz + l) * cores + c,
                ((((i + l) % nx) * ny + (k ^ dy)) * nz + l) * cores + (c ^ dc),
            )
            for i in range(nx)
            for k in range(ny)
            for l in range(nz)
            for c in range(cores)
        ]

    mine, others = of_head(core), of_head(1 - core)
    own = jnp.stack(
        [
            jnp.stack([lax.ppermute(mine, CTX, handed(dy, 0)), lax.ppermute(others, CTX, handed(dy, 1))])
            for dy in range(ny)
        ]
    )

    def shifted(a, d):
        return lax.ppermute(a, "ctx_2", [(k, (k + d) % nz) for k in range(nz)])

    kv_all = [own] + [None] * (nz - 1)
    for d in range(1, nz // 2):
        kv_all[d] = shifted(kv_all[d - 1], 1)
        kv_all[nz - d] = shifted(kv_all[(nz - d + 1) % nz], -1)
    far = nz // 2
    kv_all[far] = jnp.stack([shifted(kv_all[far - 1][0], 1), shifted(kv_all[far + 1][1], -1)])

    by_core = jnp.swapaxes(queries.reshape(tok_rows, cores, GROUP * HEAD_SIZE), 0, 1)
    q_send = jnp.broadcast_to(by_core[None], (nx, *by_core.shape)).reshape(
        nx * cores, tok_rows, GROUP * HEAD_SIZE
    )
    q_all = lax.all_to_all(q_send, XC, 0, 0, tiled=True)
    parts = partial_attention(meta, q_all, kv_all)
    arrived = lax.all_to_all(parts, XC, 0, 0, tiled=True)
    attended, chosen = merged_attention(scored, arrived)

    half = residual.shape[1]
    head = lax.axis_index("head")
    partial_value = jnp.dot(chosen, out_weight, preferred_element_type=jnp.float32)[:count]
    own = lax.dynamic_slice_in_dim(partial_value, head * half, half, 1)
    own = own + residual.astype(jnp.float32)
    partial_value = lax.dynamic_update_slice_in_dim(partial_value, own, head * half, 1)
    other = swap_heads(partial_value.astype(jnp.bfloat16)).astype(jnp.float32)
    hidden_all = partial_value + other
    squares = jnp.sum(hidden_all * hidden_all, axis=1, keepdims=True)
    hidden = own + lax.dynamic_slice_in_dim(other, head * half, half, 1)
    normed = (
        hidden * lax.rsqrt(squares / hidden_all.shape[1] + 1e-05) * norm_gain[None, :]
    ).astype(jnp.bfloat16)

    own_rows = spread(spread(normed, YZ), ("ctx_0",)).reshape(-1, half)
    other_rows = lax.ppermute(own_rows, "ctx_3", [(0, 1), (1, 0)])
    rows = own_rows.shape[0] // 2
    chips = nx * ny * nz
    vocab_rows = lm_weight.shape[1]
    my_index = ((x * ny + y) * nz + z) * cores + core
    ids = token_ids.reshape(chips, cores, count).swapaxes(0, 1).reshape(cores, 2, rows)
    ids = lax.dynamic_index_in_dim(ids, head, 1, keepdims=False) - my_index * vocab_rows

    def local_stats(normed_rows, local_ids):
        partial_logits = jnp.dot(normed_rows, lm_weight, preferred_element_type=jnp.float32)
        theirs = lax.dynamic_slice_in_dim(partial_logits, (1 - head) * rows, rows, 0)
        ours = lax.dynamic_slice_in_dim(partial_logits, head * rows, rows, 0)
        logits = ours + swap_heads(theirs.astype(jnp.bfloat16)).astype(jnp.float32)
        matches = local_ids[:, None] == jnp.arange(vocab_rows, dtype=jnp.int32)[None, :]
        target_part = jnp.sum(jnp.where(matches, logits, 0.0), axis=1)
        local_top = jnp.max(logits, axis=1)
        sum_part = jnp.sum(jnp.exp(logits - local_top[:, None]), axis=1)
        return jnp.stack([local_top, sum_part, target_part])

    ids_first = lax.dynamic_index_in_dim(ids, core, 0, keepdims=False)
    ids_second = lax.dynamic_index_in_dim(ids, 1 - core, 0, keepdims=False)
    first = local_stats(own_rows, ids_first)
    second = local_stats(other_rows, ids_second)
    stats = jnp.where(core == 0, jnp.stack([first, second]), jnp.stack([second, first]))
    by_z = spread(stats, ("ctx_2",))
    merged = merged_stats((by_z[:, :, 0], by_z[:, :, 1], by_z[:, :, 2]), 0)
    by_rest = spread(jnp.stack(merged), XYCH)
    by_rest = by_rest.reshape(-1, 2, 3, cores, rows)
    top, total, target = merged_stats((by_rest[:, :, 0], by_rest[:, :, 1], by_rest[:, :, 2]), 0)
    log_probs = (target - top - jnp.log(total)).reshape(2, cores, rows // count, count)
    log_probs = log_probs.swapaxes(1, 2).reshape(chips * cores * count)
    ratio = jnp.exp(jnp.clip(log_probs - old_logp, -4.0, 4.0))
    token_loss = -jnp.minimum(ratio * advantage, jnp.clip(ratio, 0.8, 1.2) * advantage)
    return (attended, log_probs, token_loss)


def solution(mesh):
    finer = Mesh(mesh.devices.reshape(4, 2, 8, 2, mesh.shape["head"]), AXES)
    ctx = AXES[:4]
    placed = (
        P(ctx, "head"),
        P(ctx, "head"),
        P(ctx, "head"),
        P(),
        P(ctx),
        P(ctx, "head"),
        P("head"),
        P("head", None),
        P("head", ctx),
        P(),
        P(),
        P(),
    )
    return jax.shard_map(
        per_device,
        mesh=finer,
        in_specs=placed,
        out_specs=(P(ctx, "head"), P(), P()),
        check_vma=False,
    )
```

```python
import functools

import jax
import jax.numpy as jnp
from jax import lax
from jax.experimental import pallas as pl
from jax.experimental.pallas import tpu as pltpu
from jax.sharding import Mesh
from jax.sharding import PartitionSpec as P


HEAD_SIZE = 128
GROUP = 4
DOCS = 8
AXES = ("ctx_0", "ctx_1", "ctx_2", "ctx_3", "head")
CTX = AXES[:4]
XC = ("ctx_0", "ctx_3")
YZ = ("ctx_1", "ctx_2")
XYCH = ("ctx_0", "ctx_1", "ctx_3", "head")

LOG2E = 1.4426950408889634
SCORE_TO_LOG2 = HEAD_SIZE ** (-0.5) * LOG2E
EXTRA = 8
MASKED = -1e30
NO_TOP = -1e20


def size_of(axes):
    n = 1
    for a in axes:
        n *= lax.axis_size(a)
    return n


def spread(shard, axes):
    n = size_of(axes)
    return lax.all_to_all(
        jnp.broadcast_to(shard[None], (n, *shard.shape)), axes, 0, 0, tiled=True
    )


def swap_heads(shard):
    return lax.ppermute(shard, "head", [(0, 1), (1, 0)])


def gather_keys(meta_ref, kv_refs, k_ref, v_ref):
    x, y, z, core = [meta_ref[DOCS + n] for n in range(4)]
    groups = len(kv_refs)
    half = kv_refs[0].shape[2]
    chunk_rows = 4 * half
    v_ref[:, HEAD_SIZE:] = jnp.ones((groups * chunk_rows, HEAD_SIZE), jnp.bfloat16)
    for d in range(groups):
        place = (z - d) & (groups - 1)
        source = (x - place) & (groups // 2 - 1)
        for dy in range(2):
            base = (source * 2 + (y ^ dy)) * chunk_rows + (place // (groups // 2)) * 2 * half
            for dc in range(2):
                at = pl.multiple_of(base + (core ^ dc) * half, half)
                k_ref[pl.ds(at, half), :] = kv_refs[d][dy, dc, :, :HEAD_SIZE]
                v_ref[pl.ds(at, half), :HEAD_SIZE] = kv_refs[d][dy, dc, :, HEAD_SIZE:]


def chunk_start(meta_ref, groups, rows, i):
    return i * groups * rows + ((meta_ref[DOCS] - i // 2) & (groups // 2 - 1)) * rows


def doc_start(meta_ref, pos):
    low = jnp.zeros_like(pos)
    for d in range(DOCS):
        start = meta_ref[d]
        low = jnp.where(start <= pos, jnp.maximum(low, start), low)
    return low


def stats_of(tops, totals):
    lane = lax.broadcasted_iota(jnp.int32, tops[0].shape, 1)
    top, total = tops[0], totals[0]
    for g in range(1, GROUP):
        top = jnp.where(lane % GROUP == g, tops[g], top)
        total = jnp.where(lane % GROUP == g, totals[g], total)
    high = total.astype(jnp.bfloat16).astype(jnp.float32)
    middle = (total - high).astype(jnp.bfloat16).astype(jnp.float32)
    low = total - high - middle
    stats = jnp.where(lane < GROUP, top, high)
    stats = jnp.where(lane >= 2 * GROUP, middle, stats)
    stats = jnp.where(lane >= 3 * GROUP, low, stats)
    return jnp.where(lane >= 4 * GROUP, 0.0, stats).astype(jnp.bfloat16)


def query_kernel(scored_ref, q_ref, out_ref):
    rows = q_ref.shape[0]
    width = out_ref.shape[2]
    count = scored_ref.shape[0]
    row = lax.broadcasted_iota(jnp.int32, (EXTRA, rows), 0)
    col = lax.broadcasted_iota(jnp.int32, (EXTRA, rows), 1)
    wide = lax.broadcasted_iota(jnp.int32, (EXTRA, width), 0)
    pick = jnp.zeros((EXTRA, rows), jnp.float32)
    offsets = jnp.zeros((EXTRA, width), jnp.int32)
    for i in range(count):
        pick = jnp.where((row == i) & (col == scored_ref[i]), 1.0, pick)
        offsets = jnp.where(wide == EXTRA // 2 + i, scored_ref[i], offsets)
    pick = pick.astype(jnp.bfloat16)
    offsets = offsets.astype(jnp.float32)
    for c in range(2):
        heads = q_ref[:, c * width : (c + 1) * width]
        extra = jnp.dot(pick, heads, preferred_element_type=jnp.float32) + offsets
        for n in range(out_ref.shape[0] // 2):
            out_ref[2 * n + c, :rows] = heads
            out_ref[2 * n + c, rows:] = extra.astype(jnp.bfloat16)


def queries_to_send(scored, queries, copies):
    rows, features = queries.shape
    return pl.pallas_call(
        query_kernel,
        in_specs=[
            pl.BlockSpec(memory_space=pltpu.SMEM),
            pl.BlockSpec(memory_space=pltpu.VMEM),
        ],
        out_specs=pl.BlockSpec(memory_space=pltpu.VMEM),
        out_shape=jax.ShapeDtypeStruct((2 * copies, rows + EXTRA, features // 2), jnp.bfloat16),
        name="queries_to_send",
    )(scored, queries)


def chosen_kernel(meta_ref, q_ref, *refs):
    groups = len(refs) - 6
    kv_refs = refs[:groups]
    out_ref, k_ref, v_ref, m_ref, acc_ref, s_ref = refs[groups:]
    half = kv_refs[0].shape[2]
    rows = 2 * half
    span = groups * rows
    chunks, lines, chunk_rows = s_ref.shape
    peers = q_ref.shape[0]
    each = lines // GROUP
    y, z = meta_ref[DOCS + 1], meta_ref[DOCS + 2]
    gather_keys(meta_ref, kv_refs, k_ref, v_ref)
    wide = q_ref[...].astype(jnp.float32)
    offset = pltpu.roll(wide[:, :, :HEAD_SIZE], EXTRA // 2, 1).astype(jnp.int32)
    peer = lax.broadcasted_iota(jnp.int32, offset.shape, 0)
    pos = (2 * (peer // 2) + y) * span + z * rows + (peer % 2) * half + offset
    pos = pos.reshape(each, HEAD_SIZE)
    low = doc_start(meta_ref, pos)
    q = jnp.concatenate(
        [
            wide[:, :, g * HEAD_SIZE : (g + 1) * HEAD_SIZE].reshape(each, HEAD_SIZE)
            for g in range(GROUP)
        ]
    ).astype(jnp.bfloat16)
    pos = jnp.concatenate([pos] * GROUP)
    low = jnp.concatenate([low] * GROUP)
    m_ref[...] = jnp.full(m_ref.shape, NO_TOP, jnp.float32)
    acc_ref[...] = jnp.zeros(acc_ref.shape, jnp.float32)

    def score_step(i, carry):
        at = pl.multiple_of(i * chunk_rows, chunk_rows)
        s = lax.dot_general(
            q,
            k_ref[pl.ds(at, chunk_rows), :],
            (((1,), (1,)), ((), ())),
            preferred_element_type=jnp.float32,
        )
        base = chunk_start(meta_ref, groups, rows, i)
        top = m_ref[...]
        for h in range(chunk_rows // HEAD_SIZE):
            start = h * HEAD_SIZE
            if start >= rows:
                start += span // 2 - rows
            key = lax.broadcasted_iota(jnp.int32, pos.shape, 1) + (base + start)
            part = jnp.where(
                (key >= low) & (key <= pos), s[:, h * HEAD_SIZE : (h + 1) * HEAD_SIZE], MASKED
            )
            s_ref[i, :, h * HEAD_SIZE : (h + 1) * HEAD_SIZE] = part
            top = jnp.maximum(top, part)
        m_ref[...] = top
        return carry

    lax.fori_loop(0, chunks, score_step, 0)
    top = jnp.max(m_ref[...], axis=1, keepdims=True) * SCORE_TO_LOG2
    top = jnp.maximum(top, NO_TOP).astype(jnp.bfloat16).astype(jnp.float32)
    top = jnp.broadcast_to(top, m_ref.shape)
    m_ref[...] = top

    def weigh_step(i, carry):
        at = pl.multiple_of(i * chunk_rows, chunk_rows)
        tops = jnp.concatenate([m_ref[...]] * (chunk_rows // HEAD_SIZE), axis=1)
        p = jnp.exp2(s_ref[i] * SCORE_TO_LOG2 - tops).astype(jnp.bfloat16)
        acc_ref[...] += jnp.dot(
            p, v_ref[pl.ds(at, chunk_rows), :], preferred_element_type=jnp.float32
        )
        return carry

    lax.fori_loop(0, chunks, weigh_step, 0)
    tops, totals = [], []
    for g in range(GROUP):
        at = slice(g * each, (g + 1) * each)
        out_ref[:, :, g * HEAD_SIZE : (g + 1) * HEAD_SIZE] = (
            acc_ref[at, :HEAD_SIZE].reshape(peers, EXTRA, HEAD_SIZE).astype(jnp.bfloat16)
        )
        tops.append(m_ref[at])
        totals.append(acc_ref[at, HEAD_SIZE:])
    out_ref[:, :, GROUP * HEAD_SIZE :] = stats_of(tops, totals).reshape(peers, EXTRA, HEAD_SIZE)


def chosen_attention(meta, q_all, kv_all):
    peers, tall, width = q_all.shape
    half = tall - EXTRA
    chunk_rows = 4 * half
    keys = chunk_rows * len(kv_all)
    lines = GROUP * peers * EXTRA
    wide = width + HEAD_SIZE
    return pl.pallas_call(
        chosen_kernel,
        grid_spec=pltpu.PrefetchScalarGridSpec(
            num_scalar_prefetch=1,
            grid=(1,),
            in_specs=[pl.BlockSpec((peers, EXTRA, width), lambda j, meta: (0, half // EXTRA, 0))]
            + [pl.BlockSpec((2, 2, half, 2 * HEAD_SIZE), lambda j, meta: (0, 0, 0, 0))]
            * len(kv_all),
            out_specs=pl.BlockSpec((peers, EXTRA, wide), lambda j, meta: (0, 0, 0)),
            scratch_shapes=[
                pltpu.VMEM((keys, HEAD_SIZE), jnp.bfloat16),
                pltpu.VMEM((keys, 2 * HEAD_SIZE), jnp.bfloat16),
                pltpu.VMEM((lines, HEAD_SIZE), jnp.float32),
                pltpu.VMEM((lines, 2 * HEAD_SIZE), jnp.float32),
                pltpu.VMEM((keys // chunk_rows, lines, chunk_rows), jnp.float32),
            ],
        ),
        out_shape=jax.ShapeDtypeStruct((peers, EXTRA, wide), jnp.bfloat16),
        name="chosen_attention",
    )(meta, q_all, *kv_all)


def attention_kernel(first_block, meta_ref, q_ref, *refs):
    groups = len(refs) - 7
    kv_refs = refs[:groups]
    out_ref, k_ref, v_ref, m_ref, acc_ref, s_ref = refs[groups + 1 :]
    j = pl.program_id(0) + first_block
    half = out_ref.shape[1]
    rows = 2 * half
    chunk_rows = s_ref.shape[3]
    chunks = s_ref.shape[1]
    y, z = meta_ref[DOCS + 1], meta_ref[DOCS + 2]
    span = groups * rows

    @pl.when(j == first_block)
    def _():
        gather_keys(meta_ref, kv_refs, k_ref, v_ref)

    first_q = (2 * j + y) * span + z * rows
    last_q = first_q + rows - 1
    far = span // 2
    reach = far + rows - 1

    chunk_base = functools.partial(chunk_start, meta_ref, groups, rows)
    low_first = doc_start(meta_ref, first_q)
    low_last = doc_start(meta_ref, last_q)
    m_ref[...] = jnp.full(m_ref.shape, NO_TOP, jnp.float32)
    acc_ref[...] = jnp.zeros(acc_ref.shape, jnp.float32)
    chunk_lo, chunk_hi = jnp.int32(0), jnp.int32(0)
    for i in range(chunks):
        base = chunk_base(i)
        chunk_lo += (base + reach < low_first).astype(jnp.int32)
        chunk_hi += (base <= last_q).astype(jnp.int32)

    def score(i, masked):
        at = pl.multiple_of(i * chunk_rows, chunk_rows)
        k = k_ref[pl.ds(at, chunk_rows), :]
        if masked:
            pos = first_q + lax.broadcasted_iota(jnp.int32, (rows, 1), 0)
            low = doc_start(meta_ref, pos)
            base = chunk_base(i)
            key = lax.broadcasted_iota(jnp.int32, (rows, chunk_rows), 1)
            key = key + jnp.where(key >= rows, far - rows, 0)
            allowed = (key >= low - base) & (key <= pos - base)
        for g in range(GROUP):
            q = q_ref[:, :, g * HEAD_SIZE : (g + 1) * HEAD_SIZE].reshape(rows, HEAD_SIZE)
            s = lax.dot_general(
                q, k, (((1,), (1,)), ((), ())), preferred_element_type=jnp.float32
            )
            if masked:
                s = jnp.where(allowed, s, MASKED)
            s_ref[g, i] = s
            top = m_ref[g]
            for h in range(chunk_rows // HEAD_SIZE):
                top = jnp.maximum(top, s[:, h * HEAD_SIZE : (h + 1) * HEAD_SIZE])
            m_ref[g] = top

    def score_step(i, carry):
        base = chunk_base(i)
        free = (base >= low_last) & (base + reach <= first_q)

        @pl.when(free)
        def _():
            score(i, False)

        @pl.when(jnp.logical_not(free))
        def _():
            score(i, True)

        return carry

    lax.fori_loop(chunk_lo, chunk_hi, score_step, 0)
    for g in range(GROUP):
        top = jnp.max(m_ref[g], axis=1, keepdims=True) * SCORE_TO_LOG2
        top = jnp.maximum(top, NO_TOP).astype(jnp.bfloat16).astype(jnp.float32)
        m_ref[g] = jnp.broadcast_to(top, (rows, HEAD_SIZE))

    def weigh_step(i, carry):
        at = pl.multiple_of(i * chunk_rows, chunk_rows)
        v = v_ref[pl.ds(at, chunk_rows), :]
        for g in range(GROUP):
            top = m_ref[g]
            top = jnp.concatenate([top] * (chunk_rows // HEAD_SIZE), axis=1)
            p = jnp.exp2(s_ref[g, i] * SCORE_TO_LOG2 - top).astype(jnp.bfloat16)
            acc_ref[g] += jnp.dot(p, v, preferred_element_type=jnp.float32)
        return carry

    lax.fori_loop(chunk_lo, chunk_hi, weigh_step, 0)

    for g in range(GROUP):
        out_ref[:, :, g * HEAD_SIZE : (g + 1) * HEAD_SIZE] = (
            acc_ref[g, :, :HEAD_SIZE].astype(jnp.bfloat16).reshape(2, half, HEAD_SIZE)
        )
    stats = stats_of(
        [m_ref[g] for g in range(GROUP)], [acc_ref[g, :, HEAD_SIZE:] for g in range(GROUP)]
    )
    out_ref[:, :, GROUP * HEAD_SIZE :] = stats.reshape(2, half, HEAD_SIZE)


def partial_attention(meta, q_all, kv_all, first, number, before):
    peers, tall, width = q_all.shape
    half = tall - EXTRA
    rows = 2 * half
    chunk_rows = 2 * rows
    keys = chunk_rows * len(kv_all)
    wide = width + HEAD_SIZE
    at = lambda j, meta: (j + first, 0, 0)
    return pl.pallas_call(
        functools.partial(attention_kernel, first),
        grid_spec=pltpu.PrefetchScalarGridSpec(
            num_scalar_prefetch=1,
            grid=(number,),
            in_specs=[pl.BlockSpec((2, half, width), at)]
            + [pl.BlockSpec((2, 2, half, 2 * HEAD_SIZE), lambda j, meta: (0, 0, 0, 0))]
            * len(kv_all)
            + [pl.BlockSpec(memory_space=pl.ANY)],
            out_specs=pl.BlockSpec((2, half, wide), at),
            scratch_shapes=[
                pltpu.VMEM((keys, HEAD_SIZE), jnp.bfloat16),
                pltpu.VMEM((keys, 2 * HEAD_SIZE), jnp.bfloat16),
                pltpu.VMEM((GROUP, rows, HEAD_SIZE), jnp.float32),
                pltpu.VMEM((GROUP, rows, 2 * HEAD_SIZE), jnp.float32),
                pltpu.VMEM((GROUP, keys // chunk_rows, rows, chunk_rows), jnp.float32),
            ],
        ),
        out_shape=jax.ShapeDtypeStruct((peers, half, wide), jnp.bfloat16),
        input_output_aliases={2 + len(kv_all): 0} if first else {},
        compiler_params=pltpu.CompilerParams(dimension_semantics=("arbitrary",)),
        cost_estimate=pl.CostEstimate(
            flops=number * 5 * 10**9, bytes_accessed=4 * 10**6, transcendentals=0
        ),
        name="partial_attention",
    )(meta, q_all, *kv_all, before)


def merge_kernel(parts_ref, merged_ref):
    windows = parts_ref.shape[0] // 2
    rows = parts_ref.shape[1]
    for c in range(2):
        tops, sums = [], []
        for w in range(windows):
            st = parts_ref[2 * w + c, :, GROUP * HEAD_SIZE :].astype(jnp.float32)
            tops.append(st)
            sums.append(
                pltpu.roll(st, HEAD_SIZE - GROUP, 1)
                + pltpu.roll(st, HEAD_SIZE - 2 * GROUP, 1)
                + pltpu.roll(st, HEAD_SIZE - 3 * GROUP, 1)
            )
        top = functools.reduce(jnp.maximum, tops)
        shares = [jnp.exp2(t - top) for t in tops]
        total = functools.reduce(jnp.add, [n * share for n, share in zip(sums, shares)])
        lane = lax.broadcasted_iota(jnp.int32, total.shape, 1)
        total = jnp.where((lane < GROUP) & (total > 0.0), total, 1.0)
        shares = [share / total for share in shares]
        for g in range(GROUP):
            result = jnp.zeros((rows, HEAD_SIZE), jnp.float32)
            for w in range(windows):
                part = parts_ref[2 * w + c, :, g * HEAD_SIZE : (g + 1) * HEAD_SIZE]
                result = result + shares[w][:, g : g + 1] * part.astype(jnp.float32)
            at = (c * GROUP + g) * HEAD_SIZE
            merged_ref[:, at : at + HEAD_SIZE] = result.astype(jnp.bfloat16)


def merged_attention(parts):
    rows = parts.shape[1]
    return pl.pallas_call(
        merge_kernel,
        in_specs=[pl.BlockSpec(memory_space=pltpu.VMEM)],
        out_specs=pl.BlockSpec(memory_space=pltpu.VMEM),
        out_shape=jax.ShapeDtypeStruct((rows, 2 * GROUP * HEAD_SIZE), jnp.bfloat16),
    )(parts)


def merged_stats(stats, axis):
    tops, sums, targets = stats
    top = jnp.max(tops, axis=axis)
    total = jnp.sum(sums * jnp.exp(tops - jnp.expand_dims(top, axis)), axis=axis)
    return (top, total, jnp.sum(targets, axis=axis))


def per_device(
    queries,
    rotated_keys,
    value_matrix,
    doc_lengths,
    scored,
    residual,
    norm_gain,
    out_weight,
    lm_weight,
    token_ids,
    old_logp,
    advantage,
):
    count = scored.shape[0]
    nx, ny, nz, cores = [lax.axis_size(a) for a in CTX]
    x, y, z, core = [lax.axis_index(a) for a in CTX]
    doc_starts = jnp.cumsum(doc_lengths) - doc_lengths
    meta = jnp.concatenate(
        [doc_starts.astype(jnp.int32), jnp.stack([x, y, z, core]).astype(jnp.int32)]
    )

    def of_head(c):
        at = c * HEAD_SIZE
        return jnp.concatenate(
            [
                lax.dynamic_slice_in_dim(rotated_keys, at, HEAD_SIZE, 1),
                lax.dynamic_slice_in_dim(value_matrix, at, HEAD_SIZE, 1),
            ],
            axis=1,
        )

    def handed(dy, dc):
        return [
            (
                ((i * ny + k) * nz + l) * cores + c,
                ((((i + l) % nx) * ny + (k ^ dy)) * nz + l) * cores + (c ^ dc),
            )
            for i in range(nx)
            for k in range(ny)
            for l in range(nz)
            for c in range(cores)
        ]

    mine, others = of_head(core), of_head(1 - core)
    own = jnp.stack(
        [
            jnp.stack([lax.ppermute(mine, CTX, handed(dy, 0)), lax.ppermute(others, CTX, handed(dy, 1))])
            for dy in range(ny)
        ]
    )

    def shifted(a, d):
        return lax.ppermute(a, "ctx_2", [(k, (k + d) % nz) for k in range(nz)])

    kv_all = [own] + [None] * (nz - 1)
    for d in range(1, nz // 2):
        kv_all[d] = shifted(kv_all[d - 1], 1)
        kv_all[nz - d] = shifted(kv_all[(nz - d + 1) % nz], -1)
    far = nz // 2
    kv_all[far] = jnp.stack([shifted(kv_all[far - 1][0], 1), shifted(kv_all[far + 1][1], -1)])

    q_send = queries_to_send(scored, queries, nx)
    q_all = lax.all_to_all(q_send, XC, 0, 0, tiled=True)
    few = chosen_attention(meta, q_all, kv_all)
    few = lax.all_to_all(few, XC, 0, 0, tiled=True)
    chosen = merged_attention(few)
    parts = partial_attention(meta, q_all, kv_all, 0, nx // 2, q_all)
    parts = partial_attention(meta, q_all, kv_all, nx // 2, nx - nx // 2, parts)
    arrived = lax.all_to_all(parts, XC, 0, 0, tiled=True)
    attended = merged_attention(arrived)

    half = residual.shape[1]
    head = lax.axis_index("head")
    partial_value = jnp.dot(chosen, out_weight, preferred_element_type=jnp.float32)[:count]
    own = lax.dynamic_slice_in_dim(partial_value, head * half, half, 1)
    own = own + residual.astype(jnp.float32)
    partial_value = lax.dynamic_update_slice_in_dim(partial_value, own, head * half, 1)
    other = swap_heads(partial_value.astype(jnp.bfloat16)).astype(jnp.float32)
    hidden_all = partial_value + other
    squares = jnp.sum(hidden_all * hidden_all, axis=1, keepdims=True)
    hidden = own + lax.dynamic_slice_in_dim(other, head * half, half, 1)
    normed = (
        hidden * lax.rsqrt(squares / hidden_all.shape[1] + 1e-05) * norm_gain[None, :]
    ).astype(jnp.bfloat16)

    along_yz = spread(normed, YZ)
    own_rows = spread(along_yz, ("ctx_0",)).reshape(-1, half)
    other_rows = lax.ppermute(own_rows, "ctx_3", [(0, 1), (1, 0)])
    rows = own_rows.shape[0] // 2
    chips = nx * ny * nz
    vocab_rows = lm_weight.shape[1]
    my_index = ((x * ny + y) * nz + z) * cores + core
    ids = token_ids.reshape(chips, cores, count).swapaxes(0, 1).reshape(cores, 2, rows)
    ids = lax.dynamic_index_in_dim(ids, head, 1, keepdims=False) - my_index * vocab_rows

    def local_stats(normed_rows, local_ids):
        partial_logits = jnp.dot(normed_rows, lm_weight, preferred_element_type=jnp.float32)
        theirs = lax.dynamic_slice_in_dim(partial_logits, (1 - head) * rows, rows, 0)
        ours = lax.dynamic_slice_in_dim(partial_logits, head * rows, rows, 0)
        logits = ours + swap_heads(theirs.astype(jnp.bfloat16)).astype(jnp.float32)
        matches = local_ids[:, None] == jnp.arange(vocab_rows, dtype=jnp.int32)[None, :]
        target_part = jnp.sum(jnp.where(matches, logits, 0.0), axis=1)
        local_top = jnp.max(logits, axis=1)
        sum_part = jnp.sum(jnp.exp(logits - local_top[:, None]), axis=1)
        return jnp.stack([local_top, sum_part, target_part])

    ids_first = lax.dynamic_index_in_dim(ids, core, 0, keepdims=False)
    ids_second = lax.dynamic_index_in_dim(ids, 1 - core, 0, keepdims=False)
    first = local_stats(own_rows, ids_first)
    second = local_stats(other_rows, ids_second)
    stats = jnp.where(core == 0, jnp.stack([first, second]), jnp.stack([second, first]))
    by_z = spread(stats, ("ctx_2",))
    merged = merged_stats((by_z[:, :, 0], by_z[:, :, 1], by_z[:, :, 2]), 0)
    by_rest = spread(jnp.stack(merged), XYCH)
    by_rest = by_rest.reshape(-1, 2, 3, cores, rows)
    top, total, target = merged_stats((by_rest[:, :, 0], by_rest[:, :, 1], by_rest[:, :, 2]), 0)
    log_probs = (target - top - jnp.log(total)).reshape(2, cores, rows // count, count)
    log_probs = log_probs.swapaxes(1, 2).reshape(chips * cores * count)
    ratio = jnp.exp(jnp.clip(log_probs - old_logp, -4.0, 4.0))
    token_loss = -jnp.minimum(ratio * advantage, jnp.clip(ratio, 0.8, 1.2) * advantage)
    return (attended, log_probs, token_loss)


def solution(mesh):
    finer = Mesh(mesh.devices.reshape(4, 2, 8, 2, mesh.shape["head"]), AXES)
    ctx = AXES[:4]
    placed = (
        P(ctx, "head"),
        P(ctx, "head"),
        P(ctx, "head"),
        P(),
        P(ctx),
        P(ctx, "head"),
        P("head"),
        P("head", None),
        P("head", ctx),
        P(),
        P(),
        P(),
    )

    return jax.shard_map(
        per_device,
        mesh=finer,
        in_specs=placed,
        out_specs=(P(ctx, "head"), P(), P()),
        check_vma=False,
    )
```

```python
import functools

import jax
import jax.numpy as jnp
from jax import lax
from jax.experimental import pallas as pl
from jax.experimental.pallas import tpu as pltpu
from jax.sharding import Mesh
from jax.sharding import PartitionSpec as P


HEAD_SIZE = 128
GROUP = 4
DOCS = 8
AXES = ("ctx_0", "ctx_1", "ctx_2", "ctx_3", "head")
CTX = AXES[:4]
XC = ("ctx_0", "ctx_3")
YZ = ("ctx_1", "ctx_2")
XYCH = ("ctx_0", "ctx_1", "ctx_3", "head")

LOG2E = 1.4426950408889634
SCORE_TO_LOG2 = HEAD_SIZE ** (-0.5) * LOG2E
EXTRA = 8
MASKED = -1e30
NO_TOP = -1e20


def size_of(axes):
    n = 1
    for a in axes:
        n *= lax.axis_size(a)
    return n


def spread(shard, axes):
    n = size_of(axes)
    return lax.all_to_all(
        jnp.broadcast_to(shard[None], (n, *shard.shape)), axes, 0, 0, tiled=True
    )


def swap_heads(shard):
    return lax.ppermute(shard, "head", [(0, 1), (1, 0)])


def gather_keys(meta_ref, kv_refs, k_ref, v_ref):
    x, y, z, core = [meta_ref[DOCS + n] for n in range(4)]
    groups = len(kv_refs)
    half = kv_refs[0].shape[2]
    chunk_rows = 4 * half
    v_ref[:, HEAD_SIZE:] = jnp.ones((groups * chunk_rows, HEAD_SIZE), jnp.bfloat16)
    for d in range(groups):
        place = (z - d) & (groups - 1)
        source = (x - place) & (groups // 2 - 1)
        for dy in range(2):
            base = (source * 2 + (y ^ dy)) * chunk_rows + (place // (groups // 2)) * 2 * half
            for dc in range(2):
                at = pl.multiple_of(base + (core ^ dc) * half, half)
                k_ref[pl.ds(at, half), :] = kv_refs[d][dy, dc, :, :HEAD_SIZE]
                v_ref[pl.ds(at, half), :HEAD_SIZE] = kv_refs[d][dy, dc, :, HEAD_SIZE:]


def chunk_start(meta_ref, groups, rows, i):
    return i * groups * rows + ((meta_ref[DOCS] - i // 2) & (groups // 2 - 1)) * rows


def doc_start(meta_ref, pos):
    low = jnp.zeros_like(pos)
    for d in range(DOCS):
        start = meta_ref[d]
        low = jnp.where(start <= pos, jnp.maximum(low, start), low)
    return low


def stats_of(tops, totals):
    lane = lax.broadcasted_iota(jnp.int32, tops[0].shape, 1)
    top, total = tops[0], totals[0]
    for g in range(1, GROUP):
        top = jnp.where(lane % GROUP == g, tops[g], top)
        total = jnp.where(lane % GROUP == g, totals[g], total)
    high = total.astype(jnp.bfloat16).astype(jnp.float32)
    middle = (total - high).astype(jnp.bfloat16).astype(jnp.float32)
    low = total - high - middle
    stats = jnp.where(lane < GROUP, top, high)
    stats = jnp.where(lane >= 2 * GROUP, middle, stats)
    stats = jnp.where(lane >= 3 * GROUP, low, stats)
    return jnp.where(lane >= 4 * GROUP, 0.0, stats).astype(jnp.bfloat16)


def query_kernel(scored_ref, q_ref, out_ref):
    rows = q_ref.shape[0]
    width = out_ref.shape[2]
    count = scored_ref.shape[0]
    row = lax.broadcasted_iota(jnp.int32, (EXTRA, rows), 0)
    col = lax.broadcasted_iota(jnp.int32, (EXTRA, rows), 1)
    wide = lax.broadcasted_iota(jnp.int32, (EXTRA, width), 0)
    pick = jnp.zeros((EXTRA, rows), jnp.float32)
    offsets = jnp.zeros((EXTRA, width), jnp.int32)
    for i in range(count):
        pick = jnp.where((row == i) & (col == scored_ref[i]), 1.0, pick)
        offsets = jnp.where(wide == EXTRA // 2 + i, scored_ref[i], offsets)
    pick = pick.astype(jnp.bfloat16)
    offsets = offsets.astype(jnp.float32)
    for c in range(2):
        heads = q_ref[:, c * width : (c + 1) * width]
        extra = jnp.dot(pick, heads, preferred_element_type=jnp.float32) + offsets
        for n in range(out_ref.shape[0] // 2):
            out_ref[2 * n + c, :rows] = heads
            out_ref[2 * n + c, rows:] = extra.astype(jnp.bfloat16)


def queries_to_send(scored, queries, copies):
    rows, features = queries.shape
    return pl.pallas_call(
        query_kernel,
        in_specs=[
            pl.BlockSpec(memory_space=pltpu.SMEM),
            pl.BlockSpec(memory_space=pltpu.VMEM),
        ],
        out_specs=pl.BlockSpec(memory_space=pltpu.VMEM),
        out_shape=jax.ShapeDtypeStruct((2 * copies, rows + EXTRA, features // 2), jnp.bfloat16),
        name="queries_to_send",
    )(scored, queries)


def chosen_kernel(meta_ref, q_ref, *refs):
    groups = len(refs) - 6
    kv_refs = refs[:groups]
    out_ref, k_ref, v_ref, m_ref, acc_ref, s_ref = refs[groups:]
    half = kv_refs[0].shape[2]
    rows = 2 * half
    span = groups * rows
    chunks, lines, chunk_rows = s_ref.shape
    peers = q_ref.shape[0]
    each = lines // GROUP
    y, z = meta_ref[DOCS + 1], meta_ref[DOCS + 2]
    gather_keys(meta_ref, kv_refs, k_ref, v_ref)
    wide = q_ref[...].astype(jnp.float32)
    offset = pltpu.roll(wide[:, :, :HEAD_SIZE], EXTRA // 2, 1).astype(jnp.int32)
    peer = lax.broadcasted_iota(jnp.int32, offset.shape, 0)
    pos = (2 * (peer // 2) + y) * span + z * rows + (peer % 2) * half + offset
    pos = pos.reshape(each, HEAD_SIZE)
    low = doc_start(meta_ref, pos)
    q = jnp.concatenate(
        [
            wide[:, :, g * HEAD_SIZE : (g + 1) * HEAD_SIZE].reshape(each, HEAD_SIZE)
            for g in range(GROUP)
        ]
    ).astype(jnp.bfloat16)
    pos = jnp.concatenate([pos] * GROUP)
    low = jnp.concatenate([low] * GROUP)
    m_ref[...] = jnp.full(m_ref.shape, NO_TOP, jnp.float32)
    acc_ref[...] = jnp.zeros(acc_ref.shape, jnp.float32)

    def score_step(i, carry):
        at = pl.multiple_of(i * chunk_rows, chunk_rows)
        s = lax.dot_general(
            q,
            k_ref[pl.ds(at, chunk_rows), :],
            (((1,), (1,)), ((), ())),
            preferred_element_type=jnp.float32,
        )
        base = chunk_start(meta_ref, groups, rows, i)
        top = m_ref[...]
        for h in range(chunk_rows // HEAD_SIZE):
            start = h * HEAD_SIZE
            if start >= rows:
                start += span // 2 - rows
            key = lax.broadcasted_iota(jnp.int32, pos.shape, 1) + (base + start)
            part = jnp.where(
                (key >= low) & (key <= pos), s[:, h * HEAD_SIZE : (h + 1) * HEAD_SIZE], MASKED
            )
            s_ref[i, :, h * HEAD_SIZE : (h + 1) * HEAD_SIZE] = part
            top = jnp.maximum(top, part)
        m_ref[...] = top
        return carry

    lax.fori_loop(0, chunks, score_step, 0)
    top = jnp.max(m_ref[...], axis=1, keepdims=True) * SCORE_TO_LOG2
    top = jnp.maximum(top, NO_TOP).astype(jnp.bfloat16).astype(jnp.float32)
    top = jnp.broadcast_to(top, m_ref.shape)
    m_ref[...] = top

    def weigh_step(i, carry):
        at = pl.multiple_of(i * chunk_rows, chunk_rows)
        tops = jnp.concatenate([m_ref[...]] * (chunk_rows // HEAD_SIZE), axis=1)
        p = jnp.exp2(s_ref[i] * SCORE_TO_LOG2 - tops).astype(jnp.bfloat16)
        acc_ref[...] += jnp.dot(
            p, v_ref[pl.ds(at, chunk_rows), :], preferred_element_type=jnp.float32
        )
        return carry

    lax.fori_loop(0, chunks, weigh_step, 0)
    tops, totals = [], []
    for g in range(GROUP):
        at = slice(g * each, (g + 1) * each)
        out_ref[:, :, g * HEAD_SIZE : (g + 1) * HEAD_SIZE] = (
            acc_ref[at, :HEAD_SIZE].reshape(peers, EXTRA, HEAD_SIZE).astype(jnp.bfloat16)
        )
        tops.append(m_ref[at])
        totals.append(acc_ref[at, HEAD_SIZE:])
    out_ref[:, :, GROUP * HEAD_SIZE :] = stats_of(tops, totals).reshape(peers, EXTRA, HEAD_SIZE)


def chosen_attention(meta, q_all, kv_all):
    peers, tall, width = q_all.shape
    half = tall - EXTRA
    chunk_rows = 4 * half
    keys = chunk_rows * len(kv_all)
    lines = GROUP * peers * EXTRA
    wide = width + HEAD_SIZE
    return pl.pallas_call(
        chosen_kernel,
        grid_spec=pltpu.PrefetchScalarGridSpec(
            num_scalar_prefetch=1,
            grid=(1,),
            in_specs=[pl.BlockSpec((peers, EXTRA, width), lambda j, meta: (0, half // EXTRA, 0))]
            + [pl.BlockSpec((2, 2, half, 2 * HEAD_SIZE), lambda j, meta: (0, 0, 0, 0))]
            * len(kv_all),
            out_specs=pl.BlockSpec((peers, EXTRA, wide), lambda j, meta: (0, 0, 0)),
            scratch_shapes=[
                pltpu.VMEM((keys, HEAD_SIZE), jnp.bfloat16),
                pltpu.VMEM((keys, 2 * HEAD_SIZE), jnp.bfloat16),
                pltpu.VMEM((lines, HEAD_SIZE), jnp.float32),
                pltpu.VMEM((lines, 2 * HEAD_SIZE), jnp.float32),
                pltpu.VMEM((keys // chunk_rows, lines, chunk_rows), jnp.float32),
            ],
        ),
        out_shape=jax.ShapeDtypeStruct((peers, EXTRA, wide), jnp.bfloat16),
        name="chosen_attention",
    )(meta, q_all, *kv_all)


def attention_kernel(first_block, meta_ref, q_ref, *refs):
    groups = len(refs) - 7
    kv_refs = refs[:groups]
    out_ref, k_ref, v_ref, m_ref, acc_ref, s_ref = refs[groups + 1 :]
    j = pl.program_id(0) + first_block
    half = out_ref.shape[1]
    rows = 2 * half
    chunk_rows = s_ref.shape[3]
    chunks = s_ref.shape[1]
    y, z = meta_ref[DOCS + 1], meta_ref[DOCS + 2]
    span = groups * rows

    @pl.when(j == first_block)
    def _():
        gather_keys(meta_ref, kv_refs, k_ref, v_ref)

    first_q = (2 * j + y) * span + z * rows
    last_q = first_q + rows - 1
    far = span // 2
    reach = far + rows - 1

    chunk_base = functools.partial(chunk_start, meta_ref, groups, rows)
    low_first = doc_start(meta_ref, first_q)
    low_last = doc_start(meta_ref, last_q)
    m_ref[...] = jnp.full(m_ref.shape, NO_TOP, jnp.float32)
    acc_ref[...] = jnp.zeros(acc_ref.shape, jnp.float32)
    chunk_lo, chunk_hi = jnp.int32(0), jnp.int32(0)
    for i in range(chunks):
        base = chunk_base(i)
        chunk_lo += (base + reach < low_first).astype(jnp.int32)
        chunk_hi += (base <= last_q).astype(jnp.int32)

    def score(i, masked):
        at = pl.multiple_of(i * chunk_rows, chunk_rows)
        k = k_ref[pl.ds(at, chunk_rows), :]
        if masked:
            pos = first_q + lax.broadcasted_iota(jnp.int32, (rows, 1), 0)
            low = doc_start(meta_ref, pos)
            base = chunk_base(i)
            key = lax.broadcasted_iota(jnp.int32, (rows, chunk_rows), 1)
            key = key + jnp.where(key >= rows, far - rows, 0)
            allowed = (key >= low - base) & (key <= pos - base)
        for g in range(GROUP):
            q = q_ref[:, :, g * HEAD_SIZE : (g + 1) * HEAD_SIZE].reshape(rows, HEAD_SIZE)
            s = lax.dot_general(
                q, k, (((1,), (1,)), ((), ())), preferred_element_type=jnp.float32
            )
            if masked:
                s = jnp.where(allowed, s, MASKED)
            s_ref[g, i] = s
            top = m_ref[g]
            for h in range(chunk_rows // HEAD_SIZE):
                top = jnp.maximum(top, s[:, h * HEAD_SIZE : (h + 1) * HEAD_SIZE])
            m_ref[g] = top

    def score_step(i, carry):
        base = chunk_base(i)
        free = (base >= low_last) & (base + reach <= first_q)

        @pl.when(free)
        def _():
            score(i, False)

        @pl.when(jnp.logical_not(free))
        def _():
            score(i, True)

        return carry

    lax.fori_loop(chunk_lo, chunk_hi, score_step, 0)
    for g in range(GROUP):
        top = jnp.max(m_ref[g], axis=1, keepdims=True) * SCORE_TO_LOG2
        top = jnp.maximum(top, NO_TOP).astype(jnp.bfloat16).astype(jnp.float32)
        m_ref[g] = jnp.broadcast_to(top, (rows, HEAD_SIZE))

    def weigh_step(i, carry):
        at = pl.multiple_of(i * chunk_rows, chunk_rows)
        v = v_ref[pl.ds(at, chunk_rows), :]
        for g in range(GROUP):
            top = m_ref[g]
            top = jnp.concatenate([top] * (chunk_rows // HEAD_SIZE), axis=1)
            p = jnp.exp2(s_ref[g, i] * SCORE_TO_LOG2 - top).astype(jnp.bfloat16)
            acc_ref[g] += jnp.dot(p, v, preferred_element_type=jnp.float32)
        return carry

    lax.fori_loop(chunk_lo, chunk_hi, weigh_step, 0)

    for g in range(GROUP):
        out_ref[:, :, g * HEAD_SIZE : (g + 1) * HEAD_SIZE] = (
            acc_ref[g, :, :HEAD_SIZE].astype(jnp.bfloat16).reshape(2, half, HEAD_SIZE)
        )
    stats = stats_of(
        [m_ref[g] for g in range(GROUP)], [acc_ref[g, :, HEAD_SIZE:] for g in range(GROUP)]
    )
    out_ref[:, :, GROUP * HEAD_SIZE :] = stats.reshape(2, half, HEAD_SIZE)


def partial_attention(meta, q_all, kv_all, first, number, before):
    peers, tall, width = q_all.shape
    half = tall - EXTRA
    rows = 2 * half
    chunk_rows = 2 * rows
    keys = chunk_rows * len(kv_all)
    wide = width + HEAD_SIZE
    at = lambda j, meta: (j + first, 0, 0)
    return pl.pallas_call(
        functools.partial(attention_kernel, first),
        grid_spec=pltpu.PrefetchScalarGridSpec(
            num_scalar_prefetch=1,
            grid=(number,),
            in_specs=[pl.BlockSpec((2, half, width), at)]
            + [pl.BlockSpec((2, 2, half, 2 * HEAD_SIZE), lambda j, meta: (0, 0, 0, 0))]
            * len(kv_all)
            + [pl.BlockSpec(memory_space=pl.ANY)],
            out_specs=pl.BlockSpec((2, half, wide), at),
            scratch_shapes=[
                pltpu.VMEM((keys, HEAD_SIZE), jnp.bfloat16),
                pltpu.VMEM((keys, 2 * HEAD_SIZE), jnp.bfloat16),
                pltpu.VMEM((GROUP, rows, HEAD_SIZE), jnp.float32),
                pltpu.VMEM((GROUP, rows, 2 * HEAD_SIZE), jnp.float32),
                pltpu.VMEM((GROUP, keys // chunk_rows, rows, chunk_rows), jnp.float32),
            ],
        ),
        out_shape=jax.ShapeDtypeStruct((peers, half, wide), jnp.bfloat16),
        input_output_aliases={2 + len(kv_all): 0} if first else {},
        compiler_params=pltpu.CompilerParams(dimension_semantics=("arbitrary",)),
        cost_estimate=pl.CostEstimate(
            flops=number * 5 * 10**9, bytes_accessed=4 * 10**6, transcendentals=0
        ),
        name="partial_attention",
    )(meta, q_all, *kv_all, before)


def merge_kernel(parts_ref, merged_ref):
    windows = parts_ref.shape[0] // 2
    rows = parts_ref.shape[1]
    for c in range(2):
        tops, sums = [], []
        for w in range(windows):
            st = parts_ref[2 * w + c, :, GROUP * HEAD_SIZE :].astype(jnp.float32)
            tops.append(st)
            sums.append(
                pltpu.roll(st, HEAD_SIZE - GROUP, 1)
                + pltpu.roll(st, HEAD_SIZE - 2 * GROUP, 1)
                + pltpu.roll(st, HEAD_SIZE - 3 * GROUP, 1)
            )
        top = functools.reduce(jnp.maximum, tops)
        shares = [jnp.exp2(t - top) for t in tops]
        total = functools.reduce(jnp.add, [n * share for n, share in zip(sums, shares)])
        lane = lax.broadcasted_iota(jnp.int32, total.shape, 1)
        total = jnp.where((lane < GROUP) & (total > 0.0), total, 1.0)
        shares = [share / total for share in shares]
        for g in range(GROUP):
            result = jnp.zeros((rows, HEAD_SIZE), jnp.float32)
            for w in range(windows):
                part = parts_ref[2 * w + c, :, g * HEAD_SIZE : (g + 1) * HEAD_SIZE]
                result = result + shares[w][:, g : g + 1] * part.astype(jnp.float32)
            at = (c * GROUP + g) * HEAD_SIZE
            merged_ref[:, at : at + HEAD_SIZE] = result.astype(jnp.bfloat16)


def merged_attention(parts):
    rows = parts.shape[1]
    return pl.pallas_call(
        merge_kernel,
        in_specs=[pl.BlockSpec(memory_space=pltpu.VMEM)],
        out_specs=pl.BlockSpec(memory_space=pltpu.VMEM),
        out_shape=jax.ShapeDtypeStruct((rows, 2 * GROUP * HEAD_SIZE), jnp.bfloat16),
    )(parts)


def merged_stats(stats, axis):
    tops, sums, targets = stats
    top = jnp.max(tops, axis=axis)
    total = jnp.sum(sums * jnp.exp(tops - jnp.expand_dims(top, axis)), axis=axis)
    return (top, total, jnp.sum(targets, axis=axis))


def per_device(
    queries,
    rotated_keys,
    value_matrix,
    doc_lengths,
    scored,
    residual,
    norm_gain,
    out_weight,
    lm_weight,
    token_ids,
    old_logp,
    advantage,
):
    tok_rows = queries.shape[0]
    count = scored.shape[0]
    nx, ny, nz, cores = [lax.axis_size(a) for a in CTX]
    x, y, z, core = [lax.axis_index(a) for a in CTX]
    doc_starts = jnp.cumsum(doc_lengths) - doc_lengths
    meta = jnp.concatenate(
        [doc_starts.astype(jnp.int32), jnp.stack([x, y, z, core]).astype(jnp.int32)]
    )

    def of_head(c):
        at = c * HEAD_SIZE
        return jnp.concatenate(
            [
                lax.dynamic_slice_in_dim(rotated_keys, at, HEAD_SIZE, 1),
                lax.dynamic_slice_in_dim(value_matrix, at, HEAD_SIZE, 1),
            ],
            axis=1,
        )

    def handed(dy, dc):
        return [
            (
                ((i * ny + k) * nz + l) * cores + c,
                ((((i + l) % nx) * ny + (k ^ dy)) * nz + l) * cores + (c ^ dc),
            )
            for i in range(nx)
            for k in range(ny)
            for l in range(nz)
            for c in range(cores)
        ]

    mine, others = of_head(core), of_head(1 - core)
    pieces = []
    for dy in range(ny):
        for dc in range(cores):
            pieces.append(lax.ppermute(others if dc else mine, CTX, handed(dy, dc)))
    own = jnp.stack(pieces).reshape(ny, cores, tok_rows, 2 * HEAD_SIZE)

    def shifted(a, d):
        return lax.ppermute(a, "ctx_2", [(k, (k + d) % nz) for k in range(nz)])

    far = nz // 2
    kv_all = [own] + [None] * (nz - 1)
    for d in range(1, far):
        kv_all[d] = shifted(kv_all[d - 1], 1)
        kv_all[nz - d] = shifted(kv_all[(nz - d + 1) % nz], -1)
    kv_all[far] = jnp.stack([shifted(kv_all[far - 1][0], 1), shifted(kv_all[far + 1][1], -1)])
    q_send = queries_to_send(scored, queries, nx)
    q_all = lax.all_to_all(q_send, XC, 0, 0, tiled=True)
    few = chosen_attention(meta, q_all, kv_all)
    few = lax.all_to_all(few, XC, 0, 0, tiled=True)
    chosen = merged_attention(few)
    parts = q_all
    for n in range(nx):
        parts = partial_attention(meta, q_all, kv_all, n, 1, parts)
    arrived = lax.all_to_all(parts, XC, 0, 0, tiled=True)
    attended = merged_attention(arrived)

    half = residual.shape[1]
    head = lax.axis_index("head")
    partial_value = jnp.dot(chosen, out_weight, preferred_element_type=jnp.float32)[:count]
    own = lax.dynamic_slice_in_dim(partial_value, head * half, half, 1)
    own = own + residual.astype(jnp.float32)
    partial_value = lax.dynamic_update_slice_in_dim(partial_value, own, head * half, 1)
    other = swap_heads(partial_value.astype(jnp.bfloat16)).astype(jnp.float32)
    hidden_all = partial_value + other
    squares = jnp.sum(hidden_all * hidden_all, axis=1, keepdims=True)
    hidden = own + lax.dynamic_slice_in_dim(other, head * half, half, 1)
    normed = (
        hidden * lax.rsqrt(squares / hidden_all.shape[1] + 1e-05) * norm_gain[None, :]
    ).astype(jnp.bfloat16)

    along_yz = spread(normed, YZ)
    own_rows = spread(along_yz, ("ctx_0",)).reshape(-1, half)
    other_rows = lax.ppermute(own_rows, "ctx_3", [(0, 1), (1, 0)])
    rows = own_rows.shape[0] // 2
    chips = nx * ny * nz
    vocab_rows = lm_weight.shape[1]
    my_index = ((x * ny + y) * nz + z) * cores + core
    ids = token_ids.reshape(chips, cores, count).swapaxes(0, 1).reshape(cores, 2, rows)
    ids = lax.dynamic_index_in_dim(ids, head, 1, keepdims=False) - my_index * vocab_rows

    def local_stats(normed_rows, local_ids):
        partial_logits = jnp.dot(normed_rows, lm_weight, preferred_element_type=jnp.float32)
        theirs = lax.dynamic_slice_in_dim(partial_logits, (1 - head) * rows, rows, 0)
        ours = lax.dynamic_slice_in_dim(partial_logits, head * rows, rows, 0)
        logits = ours + swap_heads(theirs.astype(jnp.bfloat16)).astype(jnp.float32)
        matches = local_ids[:, None] == jnp.arange(vocab_rows, dtype=jnp.int32)[None, :]
        target_part = jnp.sum(jnp.where(matches, logits, 0.0), axis=1)
        local_top = jnp.max(logits, axis=1)
        sum_part = jnp.sum(jnp.exp(logits - local_top[:, None]), axis=1)
        return jnp.stack([local_top, sum_part, target_part])

    ids_first = lax.dynamic_index_in_dim(ids, core, 0, keepdims=False)
    ids_second = lax.dynamic_index_in_dim(ids, 1 - core, 0, keepdims=False)
    first = local_stats(own_rows, ids_first)
    second = local_stats(other_rows, ids_second)
    stats = jnp.where(core == 0, jnp.stack([first, second]), jnp.stack([second, first]))
    by_z = spread(stats, ("ctx_2",))
    merged = merged_stats((by_z[:, :, 0], by_z[:, :, 1], by_z[:, :, 2]), 0)
    by_rest = spread(jnp.stack(merged), XYCH)
    by_rest = by_rest.reshape(-1, 2, 3, cores, rows)
    top, total, target = merged_stats((by_rest[:, :, 0], by_rest[:, :, 1], by_rest[:, :, 2]), 0)
    log_probs = (target - top - jnp.log(total)).reshape(2, cores, rows // count, count)
    log_probs = log_probs.swapaxes(1, 2).reshape(chips * cores * count)
    ratio = jnp.exp(jnp.clip(log_probs - old_logp, -4.0, 4.0))
    token_loss = -jnp.minimum(ratio * advantage, jnp.clip(ratio, 0.8, 1.2) * advantage)
    return (attended, log_probs, token_loss)


def solution(mesh):
    finer = Mesh(mesh.devices.reshape(4, 2, 8, 2, mesh.shape["head"]), AXES)
    ctx = AXES[:4]
    placed = (
        P(ctx, "head"),
        P(ctx, "head"),
        P(ctx, "head"),
        P(),
        P(ctx),
        P(ctx, "head"),
        P("head"),
        P("head", None),
        P("head", ctx),
        P(),
        P(),
        P(),
    )

    return jax.shard_map(
        per_device,
        mesh=finer,
        in_specs=placed,
        out_specs=(P(ctx, "head"), P(), P()),
        check_vma=False,
    )
```

```python
import functools

import jax
import jax.numpy as jnp
from jax import lax
from jax.experimental import pallas as pl
from jax.experimental.pallas import tpu as pltpu
from jax.sharding import Mesh
from jax.sharding import PartitionSpec as P


HEAD_SIZE = 128
GROUP = 4
DOCS = 8
AXES = ("ctx_0", "ctx_1", "ctx_2", "ctx_3", "head")
CTX = AXES[:4]
XC = ("ctx_0", "ctx_3")
YZ = ("ctx_1", "ctx_2")
XYCH = ("ctx_0", "ctx_1", "ctx_3", "head")

LOG2E = 1.4426950408889634
SCORE_TO_LOG2 = HEAD_SIZE ** (-0.5) * LOG2E
EXTRA = 8
MASKED = -1e30
NO_TOP = -1e20


def size_of(axes):
    n = 1
    for a in axes:
        n *= lax.axis_size(a)
    return n


def spread(shard, axes):
    n = size_of(axes)
    return lax.all_to_all(
        jnp.broadcast_to(shard[None], (n, *shard.shape)), axes, 0, 0, tiled=True
    )


def swap_heads(shard):
    return lax.ppermute(shard, "head", [(0, 1), (1, 0)])


def gather_keys(meta_ref, kv_refs, k_ref, v_ref):
    x, y, z, core = [meta_ref[DOCS + n] for n in range(4)]
    groups = len(kv_refs)
    half = kv_refs[0].shape[2]
    chunk_rows = 4 * half
    v_ref[:, HEAD_SIZE:] = jnp.ones((groups * chunk_rows, HEAD_SIZE), jnp.bfloat16)
    for d in range(groups):
        place = (z - d) & (groups - 1)
        source = (x - place) & (groups // 2 - 1)
        for dy in range(2):
            base = (source * 2 + (y ^ dy)) * chunk_rows + (place // (groups // 2)) * 2 * half
            for dc in range(2):
                at = pl.multiple_of(base + (core ^ dc) * half, half)
                k_ref[pl.ds(at, half), :] = kv_refs[d][dy, dc, :, :HEAD_SIZE]
                v_ref[pl.ds(at, half), :HEAD_SIZE] = kv_refs[d][dy, dc, :, HEAD_SIZE:]


def chunk_start(meta_ref, groups, rows, i):
    return i * groups * rows + ((meta_ref[DOCS] - i // 2) & (groups // 2 - 1)) * rows


def doc_start(meta_ref, pos):
    low = jnp.zeros_like(pos)
    for d in range(DOCS):
        start = meta_ref[d]
        low = jnp.where(start <= pos, jnp.maximum(low, start), low)
    return low


def stats_of(tops, totals):
    lane = lax.broadcasted_iota(jnp.int32, tops[0].shape, 1)
    top, total = tops[0], totals[0]
    for g in range(1, GROUP):
        top = jnp.where(lane % GROUP == g, tops[g], top)
        total = jnp.where(lane % GROUP == g, totals[g], total)
    high = total.astype(jnp.bfloat16).astype(jnp.float32)
    middle = (total - high).astype(jnp.bfloat16).astype(jnp.float32)
    low = total - high - middle
    stats = jnp.where(lane < GROUP, top, high)
    stats = jnp.where(lane >= 2 * GROUP, middle, stats)
    stats = jnp.where(lane >= 3 * GROUP, low, stats)
    return jnp.where(lane >= 4 * GROUP, 0.0, stats).astype(jnp.bfloat16)


def query_kernel(scored_ref, q_ref, out_ref):
    rows = q_ref.shape[0]
    width = out_ref.shape[2]
    count = scored_ref.shape[0]
    row = lax.broadcasted_iota(jnp.int32, (EXTRA, rows), 0)
    col = lax.broadcasted_iota(jnp.int32, (EXTRA, rows), 1)
    wide = lax.broadcasted_iota(jnp.int32, (EXTRA, width), 0)
    pick = jnp.zeros((EXTRA, rows), jnp.float32)
    offsets = jnp.zeros((EXTRA, width), jnp.int32)
    for i in range(count):
        pick = jnp.where((row == i) & (col == scored_ref[i]), 1.0, pick)
        offsets = jnp.where(wide == EXTRA // 2 + i, scored_ref[i], offsets)
    pick = pick.astype(jnp.bfloat16)
    offsets = offsets.astype(jnp.float32)
    for c in range(2):
        heads = q_ref[:, c * width : (c + 1) * width]
        extra = jnp.dot(pick, heads, preferred_element_type=jnp.float32) + offsets
        for n in range(out_ref.shape[0] // 2):
            out_ref[2 * n + c, :rows] = heads
            out_ref[2 * n + c, rows:] = extra.astype(jnp.bfloat16)


def queries_to_send(scored, queries, copies):
    rows, features = queries.shape
    return pl.pallas_call(
        query_kernel,
        in_specs=[
            pl.BlockSpec(memory_space=pltpu.SMEM),
            pl.BlockSpec(memory_space=pltpu.VMEM),
        ],
        out_specs=pl.BlockSpec(memory_space=pltpu.VMEM),
        out_shape=jax.ShapeDtypeStruct((2 * copies, rows + EXTRA, features // 2), jnp.bfloat16),
        name="queries_to_send",
    )(scored, queries)


def chosen_kernel(meta_ref, q_ref, *refs):
    groups = len(refs) - 6
    kv_refs = refs[:groups]
    out_ref, k_ref, v_ref, m_ref, acc_ref, s_ref = refs[groups:]
    half = kv_refs[0].shape[2]
    rows = 2 * half
    span = groups * rows
    chunks, lines, chunk_rows = s_ref.shape
    peers = q_ref.shape[0]
    each = lines // GROUP
    y, z = meta_ref[DOCS + 1], meta_ref[DOCS + 2]
    gather_keys(meta_ref, kv_refs, k_ref, v_ref)
    wide = q_ref[...].astype(jnp.float32)
    offset = pltpu.roll(wide[:, :, :HEAD_SIZE], EXTRA // 2, 1).astype(jnp.int32)
    peer = lax.broadcasted_iota(jnp.int32, offset.shape, 0)
    pos = (2 * (peer // 2) + y) * span + z * rows + (peer % 2) * half + offset
    pos = pos.reshape(each, HEAD_SIZE)
    low = doc_start(meta_ref, pos)
    q = jnp.concatenate(
        [
            wide[:, :, g * HEAD_SIZE : (g + 1) * HEAD_SIZE].reshape(each, HEAD_SIZE)
            for g in range(GROUP)
        ]
    ).astype(jnp.bfloat16)
    pos = jnp.concatenate([pos] * GROUP)
    low = jnp.concatenate([low] * GROUP)
    m_ref[...] = jnp.full(m_ref.shape, NO_TOP, jnp.float32)
    acc_ref[...] = jnp.zeros(acc_ref.shape, jnp.float32)

    def score_step(i, carry):
        at = pl.multiple_of(i * chunk_rows, chunk_rows)
        s = lax.dot_general(
            q,
            k_ref[pl.ds(at, chunk_rows), :],
            (((1,), (1,)), ((), ())),
            preferred_element_type=jnp.float32,
        )
        base = chunk_start(meta_ref, groups, rows, i)
        top = m_ref[...]
        for h in range(chunk_rows // HEAD_SIZE):
            start = h * HEAD_SIZE
            if start >= rows:
                start += span // 2 - rows
            key = lax.broadcasted_iota(jnp.int32, pos.shape, 1) + (base + start)
            part = jnp.where(
                (key >= low) & (key <= pos), s[:, h * HEAD_SIZE : (h + 1) * HEAD_SIZE], MASKED
            )
            s_ref[i, :, h * HEAD_SIZE : (h + 1) * HEAD_SIZE] = part
            top = jnp.maximum(top, part)
        m_ref[...] = top
        return carry

    lax.fori_loop(0, chunks, score_step, 0, unroll=True)
    top = jnp.max(m_ref[...], axis=1, keepdims=True) * SCORE_TO_LOG2
    top = jnp.maximum(top, NO_TOP).astype(jnp.bfloat16).astype(jnp.float32)
    top = jnp.broadcast_to(top, m_ref.shape)
    m_ref[...] = top

    def weigh_step(i, carry):
        at = pl.multiple_of(i * chunk_rows, chunk_rows)
        tops = jnp.concatenate([m_ref[...]] * (chunk_rows // HEAD_SIZE), axis=1)
        p = jnp.exp2(s_ref[i] * SCORE_TO_LOG2 - tops).astype(jnp.bfloat16)
        acc_ref[...] += jnp.dot(
            p, v_ref[pl.ds(at, chunk_rows), :], preferred_element_type=jnp.float32
        )
        return carry

    lax.fori_loop(0, chunks, weigh_step, 0, unroll=True)
    tops, totals = [], []
    for g in range(GROUP):
        at = slice(g * each, (g + 1) * each)
        out_ref[:, :, g * HEAD_SIZE : (g + 1) * HEAD_SIZE] = (
            acc_ref[at, :HEAD_SIZE].reshape(peers, EXTRA, HEAD_SIZE).astype(jnp.bfloat16)
        )
        tops.append(m_ref[at])
        totals.append(acc_ref[at, HEAD_SIZE:])
    out_ref[:, :, GROUP * HEAD_SIZE :] = stats_of(tops, totals).reshape(peers, EXTRA, HEAD_SIZE)


def chosen_attention(meta, q_all, kv_all):
    peers, tall, width = q_all.shape
    half = tall - EXTRA
    chunk_rows = 4 * half
    keys = chunk_rows * len(kv_all)
    lines = GROUP * peers * EXTRA
    wide = width + HEAD_SIZE
    return pl.pallas_call(
        chosen_kernel,
        grid_spec=pltpu.PrefetchScalarGridSpec(
            num_scalar_prefetch=1,
            grid=(1,),
            in_specs=[pl.BlockSpec((peers, EXTRA, width), lambda j, meta: (0, half // EXTRA, 0))]
            + [pl.BlockSpec((2, 2, half, 2 * HEAD_SIZE), lambda j, meta: (0, 0, 0, 0))]
            * len(kv_all),
            out_specs=pl.BlockSpec((peers, EXTRA, wide), lambda j, meta: (0, 0, 0)),
            scratch_shapes=[
                pltpu.VMEM((keys, HEAD_SIZE), jnp.bfloat16),
                pltpu.VMEM((keys, 2 * HEAD_SIZE), jnp.bfloat16),
                pltpu.VMEM((lines, HEAD_SIZE), jnp.float32),
                pltpu.VMEM((lines, 2 * HEAD_SIZE), jnp.float32),
                pltpu.VMEM((keys // chunk_rows, lines, chunk_rows), jnp.float32),
            ],
        ),
        out_shape=jax.ShapeDtypeStruct((peers, EXTRA, wide), jnp.bfloat16),
        name="chosen_attention",
    )(meta, q_all, *kv_all)


def attention_kernel(first_block, meta_ref, q_ref, *refs):
    groups = len(refs) - 7
    kv_refs = refs[:groups]
    out_ref, k_ref, v_ref, m_ref, acc_ref, s_ref = refs[groups + 1 :]
    j = pl.program_id(0) + first_block
    half = out_ref.shape[1]
    rows = 2 * half
    chunk_rows = s_ref.shape[3]
    chunks = s_ref.shape[1]
    y, z = meta_ref[DOCS + 1], meta_ref[DOCS + 2]
    span = groups * rows

    @pl.when(j == first_block)
    def _():
        gather_keys(meta_ref, kv_refs, k_ref, v_ref)

    first_q = (2 * j + y) * span + z * rows
    last_q = first_q + rows - 1
    far = span // 2
    reach = far + rows - 1

    chunk_base = functools.partial(chunk_start, meta_ref, groups, rows)
    low_first = doc_start(meta_ref, first_q)
    low_last = doc_start(meta_ref, last_q)
    m_ref[...] = jnp.full(m_ref.shape, NO_TOP, jnp.float32)
    acc_ref[...] = jnp.zeros(acc_ref.shape, jnp.float32)
    chunk_lo, chunk_hi = jnp.int32(0), jnp.int32(0)
    for i in range(chunks):
        base = chunk_base(i)
        chunk_lo += (base + reach < low_first).astype(jnp.int32)
        chunk_hi += (base <= last_q).astype(jnp.int32)

    def score(i, masked):
        at = pl.multiple_of(i * chunk_rows, chunk_rows)
        k = k_ref[pl.ds(at, chunk_rows), :]
        if masked:
            pos = first_q + lax.broadcasted_iota(jnp.int32, (rows, 1), 0)
            low = doc_start(meta_ref, pos)
            base = chunk_base(i)
            key = lax.broadcasted_iota(jnp.int32, (rows, chunk_rows), 1)
            key = key + jnp.where(key >= rows, far - rows, 0)
            allowed = (key >= low - base) & (key <= pos - base)
        for g in range(GROUP):
            q = q_ref[:, :, g * HEAD_SIZE : (g + 1) * HEAD_SIZE].reshape(rows, HEAD_SIZE)
            s = lax.dot_general(
                q, k, (((1,), (1,)), ((), ())), preferred_element_type=jnp.float32
            )
            if masked:
                s = jnp.where(allowed, s, MASKED)
            s_ref[g, i] = s
            top = m_ref[g]
            for h in range(chunk_rows // HEAD_SIZE):
                top = jnp.maximum(top, s[:, h * HEAD_SIZE : (h + 1) * HEAD_SIZE])
            m_ref[g] = top

    def score_step(i, carry):
        base = chunk_base(i)
        free = (base >= low_last) & (base + reach <= first_q)

        @pl.when(free)
        def _():
            score(i, False)

        @pl.when(jnp.logical_not(free))
        def _():
            score(i, True)

        return carry

    lax.fori_loop(chunk_lo, chunk_hi, score_step, 0)
    for g in range(GROUP):
        top = jnp.max(m_ref[g], axis=1, keepdims=True) * SCORE_TO_LOG2
        top = jnp.maximum(top, NO_TOP).astype(jnp.bfloat16).astype(jnp.float32)
        m_ref[g] = jnp.broadcast_to(top, (rows, HEAD_SIZE))

    def weigh_step(i, carry):
        at = pl.multiple_of(i * chunk_rows, chunk_rows)
        v = v_ref[pl.ds(at, chunk_rows), :]
        for g in range(GROUP):
            top = m_ref[g]
            top = jnp.concatenate([top] * (chunk_rows // HEAD_SIZE), axis=1)
            p = jnp.exp2(s_ref[g, i] * SCORE_TO_LOG2 - top).astype(jnp.bfloat16)
            acc_ref[g] += jnp.dot(p, v, preferred_element_type=jnp.float32)
        return carry

    lax.fori_loop(chunk_lo, chunk_hi, weigh_step, 0)

    for g in range(GROUP):
        out_ref[:, :, g * HEAD_SIZE : (g + 1) * HEAD_SIZE] = (
            acc_ref[g, :, :HEAD_SIZE].astype(jnp.bfloat16).reshape(2, half, HEAD_SIZE)
        )
    stats = stats_of(
        [m_ref[g] for g in range(GROUP)], [acc_ref[g, :, HEAD_SIZE:] for g in range(GROUP)]
    )
    out_ref[:, :, GROUP * HEAD_SIZE :] = stats.reshape(2, half, HEAD_SIZE)


def partial_attention(meta, q_all, kv_all, first, number, before):
    peers, tall, width = q_all.shape
    half = tall - EXTRA
    rows = 2 * half
    chunk_rows = 2 * rows
    keys = chunk_rows * len(kv_all)
    wide = width + HEAD_SIZE
    at = lambda j, meta: (j + first, 0, 0)
    return pl.pallas_call(
        functools.partial(attention_kernel, first),
        grid_spec=pltpu.PrefetchScalarGridSpec(
            num_scalar_prefetch=1,
            grid=(number,),
            in_specs=[pl.BlockSpec((2, half, width), at)]
            + [pl.BlockSpec((2, 2, half, 2 * HEAD_SIZE), lambda j, meta: (0, 0, 0, 0))]
            * len(kv_all)
            + [pl.BlockSpec(memory_space=pl.ANY)],
            out_specs=pl.BlockSpec((2, half, wide), at),
            scratch_shapes=[
                pltpu.VMEM((keys, HEAD_SIZE), jnp.bfloat16),
                pltpu.VMEM((keys, 2 * HEAD_SIZE), jnp.bfloat16),
                pltpu.VMEM((GROUP, rows, HEAD_SIZE), jnp.float32),
                pltpu.VMEM((GROUP, rows, 2 * HEAD_SIZE), jnp.float32),
                pltpu.VMEM((GROUP, keys // chunk_rows, rows, chunk_rows), jnp.float32),
            ],
        ),
        out_shape=jax.ShapeDtypeStruct((peers, half, wide), jnp.bfloat16),
        input_output_aliases={2 + len(kv_all): 0} if first else {},
        compiler_params=pltpu.CompilerParams(dimension_semantics=("arbitrary",)),
        cost_estimate=pl.CostEstimate(
            flops=number * 5 * 10**9, bytes_accessed=4 * 10**6, transcendentals=0
        ),
        name="partial_attention",
    )(meta, q_all, *kv_all, before)


def merge_parts(parts_ref, merged_ref):
    windows = parts_ref.shape[0] // 2
    rows = parts_ref.shape[1]
    for c in range(2):
        tops, sums = [], []
        for w in range(windows):
            st = parts_ref[2 * w + c, :, GROUP * HEAD_SIZE :].astype(jnp.float32)
            tops.append(st)
            sums.append(
                pltpu.roll(st, HEAD_SIZE - GROUP, 1)
                + pltpu.roll(st, HEAD_SIZE - 2 * GROUP, 1)
                + pltpu.roll(st, HEAD_SIZE - 3 * GROUP, 1)
            )
        top = functools.reduce(jnp.maximum, tops)
        shares = [jnp.exp2(t - top) for t in tops]
        total = functools.reduce(jnp.add, [n * share for n, share in zip(sums, shares)])
        lane = lax.broadcasted_iota(jnp.int32, total.shape, 1)
        total = jnp.where((lane < GROUP) & (total > 0.0), total, 1.0)
        shares = [share / total for share in shares]
        for g in range(GROUP):
            result = jnp.zeros((rows, HEAD_SIZE), jnp.float32)
            for w in range(windows):
                part = parts_ref[2 * w + c, :, g * HEAD_SIZE : (g + 1) * HEAD_SIZE]
                result = result + shares[w][:, g : g + 1] * part.astype(jnp.float32)
            at = (c * GROUP + g) * HEAD_SIZE
            merged_ref[:, at : at + HEAD_SIZE] = result.astype(jnp.bfloat16)


def merge_kernel(parts_ref, merged_ref):
    merge_parts(parts_ref, merged_ref)


def project_kernel(parts_ref, weight_ref, out_ref, chosen_ref):
    @pl.when(pl.program_id(0) == 0)
    def _():
        merge_parts(parts_ref, chosen_ref)

    out_ref[...] = jnp.dot(
        chosen_ref[...], weight_ref[...], preferred_element_type=jnp.float32
    )


def projected_rows(parts, out_weight):
    rows = parts.shape[1]
    features, width = out_weight.shape
    block = width // 8
    return pl.pallas_call(
        project_kernel,
        grid=(width // block,),
        in_specs=[
            pl.BlockSpec(parts.shape, lambda n: (0, 0, 0)),
            pl.BlockSpec((features, block), lambda n: (0, n)),
        ],
        out_specs=pl.BlockSpec((rows, block), lambda n: (0, n)),
        out_shape=jax.ShapeDtypeStruct((rows, width), jnp.float32),
        scratch_shapes=[pltpu.VMEM((rows, features), jnp.bfloat16)],
        compiler_params=pltpu.CompilerParams(dimension_semantics=("arbitrary",)),
        name="projected_rows",
    )(parts, out_weight)


def merged_attention(parts):
    rows = parts.shape[1]
    return pl.pallas_call(
        merge_kernel,
        in_specs=[pl.BlockSpec(memory_space=pltpu.VMEM)],
        out_specs=pl.BlockSpec(memory_space=pltpu.VMEM),
        out_shape=jax.ShapeDtypeStruct((rows, 2 * GROUP * HEAD_SIZE), jnp.bfloat16),
        name="merged_attention",
    )(parts)


def merged_stats(stats, axis):
    tops, sums, targets = stats
    top = jnp.max(tops, axis=axis)
    total = jnp.sum(sums * jnp.exp(tops - jnp.expand_dims(top, axis)), axis=axis)
    return (top, total, jnp.sum(targets, axis=axis))


def per_device(
    queries,
    rotated_keys,
    value_matrix,
    doc_lengths,
    scored,
    residual,
    norm_gain,
    out_weight,
    lm_weight,
    token_ids,
    old_logp,
    advantage,
):
    tok_rows = queries.shape[0]
    count = scored.shape[0]
    nx, ny, nz, cores = [lax.axis_size(a) for a in CTX]
    x, y, z, core = [lax.axis_index(a) for a in CTX]
    doc_starts = jnp.cumsum(doc_lengths) - doc_lengths
    meta = jnp.concatenate(
        [doc_starts.astype(jnp.int32), jnp.stack([x, y, z, core]).astype(jnp.int32)]
    )

    def of_head(c):
        at = c * HEAD_SIZE
        return jnp.concatenate(
            [
                lax.dynamic_slice_in_dim(rotated_keys, at, HEAD_SIZE, 1),
                lax.dynamic_slice_in_dim(value_matrix, at, HEAD_SIZE, 1),
            ],
            axis=1,
        )

    def handed(dy, dc):
        return [
            (
                ((i * ny + k) * nz + l) * cores + c,
                ((((i + l) % nx) * ny + (k ^ dy)) * nz + l) * cores + (c ^ dc),
            )
            for i in range(nx)
            for k in range(ny)
            for l in range(nz)
            for c in range(cores)
        ]

    mine, others = of_head(core), of_head(1 - core)
    pieces = []
    for dy in range(ny):
        for dc in range(cores):
            pieces.append(lax.ppermute(others if dc else mine, CTX, handed(dy, dc)))
    own = jnp.stack(pieces).reshape(ny, cores, tok_rows, 2 * HEAD_SIZE)

    def shifted(a, d):
        return lax.ppermute(a, "ctx_2", [(k, (k + d) % nz) for k in range(nz)])

    far = nz // 2
    kv_all = [own] + [None] * (nz - 1)
    for d in range(1, far):
        kv_all[d] = shifted(kv_all[d - 1], 1)
        kv_all[nz - d] = shifted(kv_all[(nz - d + 1) % nz], -1)
    kv_all[far] = jnp.stack([shifted(kv_all[far - 1][0], 1), shifted(kv_all[far + 1][1], -1)])
    q_send = queries_to_send(scored, queries, nx)
    q_all = lax.all_to_all(q_send, XC, 0, 0, tiled=True)
    few = chosen_attention(meta, q_all, kv_all)
    few = lax.all_to_all(few, XC, 0, 0, tiled=True)
    partial_value = projected_rows(few, out_weight)[:count]
    parts = q_all
    for first, number in ((0, 1), (1, 1), (2, nx - 2)):
        parts = partial_attention(meta, q_all, kv_all, first, number, parts)
    arrived = lax.all_to_all(parts, XC, 0, 0, tiled=True)
    attended = merged_attention(arrived)

    half = residual.shape[1]
    head = lax.axis_index("head")
    own = lax.dynamic_slice_in_dim(partial_value, head * half, half, 1)
    own = own + residual.astype(jnp.float32)
    partial_value = lax.dynamic_update_slice_in_dim(partial_value, own, head * half, 1)
    other = swap_heads(partial_value.astype(jnp.bfloat16)).astype(jnp.float32)
    hidden_all = partial_value + other
    squares = jnp.sum(hidden_all * hidden_all, axis=1, keepdims=True)
    hidden = own + lax.dynamic_slice_in_dim(other, head * half, half, 1)
    normed = (
        hidden * lax.rsqrt(squares / hidden_all.shape[1] + 1e-05) * norm_gain[None, :]
    ).astype(jnp.bfloat16)

    along_yz = spread(normed, YZ)
    own_rows = spread(along_yz, ("ctx_0",)).reshape(-1, half)
    other_rows = lax.ppermute(own_rows, "ctx_3", [(0, 1), (1, 0)])
    rows = own_rows.shape[0] // 2
    chips = nx * ny * nz
    vocab_rows = lm_weight.shape[1]
    my_index = ((x * ny + y) * nz + z) * cores + core
    ids = token_ids.reshape(chips, cores, count).swapaxes(0, 1).reshape(cores, 2, rows)
    ids = lax.dynamic_index_in_dim(ids, head, 1, keepdims=False) - my_index * vocab_rows

    def local_stats(normed_rows, local_ids):
        partial_logits = jnp.dot(
            normed_rows, lm_weight, preferred_element_type=jnp.float32
        )
        theirs = lax.dynamic_slice_in_dim(partial_logits, (1 - head) * rows, rows, 0)
        ours = lax.dynamic_slice_in_dim(partial_logits, head * rows, rows, 0)
        theirs = swap_heads(theirs.astype(jnp.bfloat16))
        logits = ours + theirs.astype(jnp.float32)
        matches = local_ids[:, None] == jnp.arange(vocab_rows, dtype=jnp.int32)[None, :]
        target_part = jnp.sum(jnp.where(matches, logits, 0.0), axis=1)
        local_top = jnp.max(logits, axis=1)
        sum_part = jnp.sum(jnp.exp(logits - local_top[:, None]), axis=1)
        return jnp.stack([local_top, sum_part, target_part])

    ids_first = lax.dynamic_index_in_dim(ids, core, 0, keepdims=False)
    ids_second = lax.dynamic_index_in_dim(ids, 1 - core, 0, keepdims=False)
    first = local_stats(own_rows, ids_first)
    second = local_stats(other_rows, ids_second)
    stats = jnp.where(core == 0, jnp.stack([first, second]), jnp.stack([second, first]))
    by_z = spread(stats, ("ctx_2",))
    merged = merged_stats((by_z[:, :, 0], by_z[:, :, 1], by_z[:, :, 2]), 0)
    by_rest = spread(jnp.stack(merged), XYCH)
    by_rest = by_rest.reshape(-1, 2, 3, cores, rows)
    top, total, target = merged_stats((by_rest[:, :, 0], by_rest[:, :, 1], by_rest[:, :, 2]), 0)
    log_probs = (target - top - jnp.log(total)).reshape(2, cores, rows // count, count)
    log_probs = log_probs.swapaxes(1, 2).reshape(chips * cores * count)
    ratio = jnp.exp(jnp.clip(log_probs - old_logp, -4.0, 4.0))
    token_loss = -jnp.minimum(ratio * advantage, jnp.clip(ratio, 0.8, 1.2) * advantage)
    return (attended, log_probs, token_loss)


def solution(mesh):
    finer = Mesh(mesh.devices.reshape(4, 2, 8, 2, mesh.shape["head"]), AXES)
    ctx = AXES[:4]
    placed = (
        P(ctx, "head"),
        P(ctx, "head"),
        P(ctx, "head"),
        P(),
        P(ctx),
        P(ctx, "head"),
        P("head"),
        P("head", None),
        P("head", ctx),
        P(),
        P(),
        P(),
    )

    return jax.shard_map(
        per_device,
        mesh=finer,
        in_specs=placed,
        out_specs=(P(ctx, "head"), P(), P()),
        check_vma=False,
    )
```

```python
import functools

import jax
import jax.numpy as jnp
from jax import lax
from jax.experimental import pallas as pl
from jax.experimental.pallas import tpu as pltpu
from jax.sharding import Mesh
from jax.sharding import PartitionSpec as P


HEAD_SIZE = 128
GROUP = 4
DOCS = 8
AXES = ("ctx_0", "ctx_1", "ctx_2", "ctx_3", "head")
CTX = AXES[:4]
XC = ("ctx_0", "ctx_3")
YZ = ("ctx_1", "ctx_2")
XYCH = ("ctx_0", "ctx_1", "ctx_3", "head")

LOG2E = 1.4426950408889634
SCORE_TO_LOG2 = HEAD_SIZE ** (-0.5) * LOG2E
EXTRA = 8
MASKED = -1e30
NO_TOP = -1e20


def size_of(axes):
    n = 1
    for a in axes:
        n *= lax.axis_size(a)
    return n


def spread(shard, axes):
    n = size_of(axes)
    return lax.all_to_all(
        jnp.broadcast_to(shard[None], (n, *shard.shape)), axes, 0, 0, tiled=True
    )


def swap_heads(shard):
    return lax.ppermute(shard, "head", [(0, 1), (1, 0)])


def gather_keys(meta_ref, kv_refs, k_ref, v_ref):
    x, y, z, core = [meta_ref[DOCS + n] for n in range(4)]
    groups = len(kv_refs)
    half = kv_refs[0].shape[2]
    chunk_rows = 4 * half
    v_ref[:, HEAD_SIZE:] = jnp.ones((groups * chunk_rows, HEAD_SIZE), jnp.bfloat16)
    for d in range(groups):
        place = (z - d) & (groups - 1)
        source = (x - place) & (groups // 2 - 1)
        for dy in range(2):
            base = (source * 2 + (y ^ dy)) * chunk_rows + (place // (groups // 2)) * 2 * half
            for dc in range(2):
                at = pl.multiple_of(base + (core ^ dc) * half, half)
                k_ref[pl.ds(at, half), :] = kv_refs[d][dy, dc, :, :HEAD_SIZE]
                v_ref[pl.ds(at, half), :HEAD_SIZE] = kv_refs[d][dy, dc, :, HEAD_SIZE:]


def chunk_start(meta_ref, groups, rows, i):
    return i * groups * rows + ((meta_ref[DOCS] - i // 2) & (groups // 2 - 1)) * rows


def doc_start(meta_ref, pos):
    low = jnp.zeros_like(pos)
    for d in range(DOCS):
        start = meta_ref[d]
        low = jnp.where(start <= pos, jnp.maximum(low, start), low)
    return low


def stats_of(tops, totals):
    lane = lax.broadcasted_iota(jnp.int32, tops[0].shape, 1)
    top, total = tops[0], totals[0]
    for g in range(1, GROUP):
        top = jnp.where(lane % GROUP == g, tops[g], top)
        total = jnp.where(lane % GROUP == g, totals[g], total)
    high = total.astype(jnp.bfloat16).astype(jnp.float32)
    middle = (total - high).astype(jnp.bfloat16).astype(jnp.float32)
    low = total - high - middle
    stats = jnp.where(lane < GROUP, top, high)
    stats = jnp.where(lane >= 2 * GROUP, middle, stats)
    stats = jnp.where(lane >= 3 * GROUP, low, stats)
    return jnp.where(lane >= 4 * GROUP, 0.0, stats).astype(jnp.bfloat16)


def query_kernel(scored_ref, q_ref, out_ref):
    rows = q_ref.shape[0]
    width = out_ref.shape[2]
    count = scored_ref.shape[0]
    row = lax.broadcasted_iota(jnp.int32, (EXTRA, rows), 0)
    col = lax.broadcasted_iota(jnp.int32, (EXTRA, rows), 1)
    wide = lax.broadcasted_iota(jnp.int32, (EXTRA, width), 0)
    pick = jnp.zeros((EXTRA, rows), jnp.float32)
    offsets = jnp.zeros((EXTRA, width), jnp.int32)
    for i in range(count):
        pick = jnp.where((row == i) & (col == scored_ref[i]), 1.0, pick)
        offsets = jnp.where(wide == EXTRA // 2 + i, scored_ref[i], offsets)
    pick = pick.astype(jnp.bfloat16)
    offsets = offsets.astype(jnp.float32)
    for c in range(2):
        heads = q_ref[:, c * width : (c + 1) * width]
        extra = jnp.dot(pick, heads, preferred_element_type=jnp.float32) + offsets
        for n in range(out_ref.shape[0] // 2):
            out_ref[2 * n + c, :rows] = heads
            out_ref[2 * n + c, rows:] = extra.astype(jnp.bfloat16)


def queries_to_send(scored, queries, copies):
    rows, features = queries.shape
    return pl.pallas_call(
        query_kernel,
        in_specs=[
            pl.BlockSpec(memory_space=pltpu.SMEM),
            pl.BlockSpec(memory_space=pltpu.VMEM),
        ],
        out_specs=pl.BlockSpec(memory_space=pltpu.VMEM),
        out_shape=jax.ShapeDtypeStruct((2 * copies, rows + EXTRA, features // 2), jnp.bfloat16),
        name="queries_to_send",
    )(scored, queries)


def chosen_kernel(meta_ref, q_ref, *refs):
    groups = len(refs) - 6
    kv_refs = refs[:groups]
    out_ref, k_ref, v_ref, m_ref, acc_ref, s_ref = refs[groups:]
    half = kv_refs[0].shape[2]
    rows = 2 * half
    span = groups * rows
    chunks, lines, chunk_rows = s_ref.shape
    peers = q_ref.shape[0]
    each = lines // GROUP
    y, z = meta_ref[DOCS + 1], meta_ref[DOCS + 2]
    gather_keys(meta_ref, kv_refs, k_ref, v_ref)
    wide = q_ref[...].astype(jnp.float32)
    offset = pltpu.roll(wide[:, :, :HEAD_SIZE], EXTRA // 2, 1).astype(jnp.int32)
    peer = lax.broadcasted_iota(jnp.int32, offset.shape, 0)
    pos = (2 * (peer // 2) + y) * span + z * rows + (peer % 2) * half + offset
    pos = pos.reshape(each, HEAD_SIZE)
    low = doc_start(meta_ref, pos)
    q = jnp.concatenate(
        [
            wide[:, :, g * HEAD_SIZE : (g + 1) * HEAD_SIZE].reshape(each, HEAD_SIZE)
            for g in range(GROUP)
        ]
    ).astype(jnp.bfloat16)
    pos = jnp.concatenate([pos] * GROUP)
    low = jnp.concatenate([low] * GROUP)
    m_ref[...] = jnp.full(m_ref.shape, NO_TOP, jnp.float32)
    acc_ref[...] = jnp.zeros(acc_ref.shape, jnp.float32)

    def score_step(i, carry):
        at = pl.multiple_of(i * chunk_rows, chunk_rows)
        s = lax.dot_general(
            q,
            k_ref[pl.ds(at, chunk_rows), :],
            (((1,), (1,)), ((), ())),
            preferred_element_type=jnp.float32,
        )
        base = chunk_start(meta_ref, groups, rows, i)
        top = m_ref[...]
        for h in range(chunk_rows // HEAD_SIZE):
            start = h * HEAD_SIZE
            if start >= rows:
                start += span // 2 - rows
            key = lax.broadcasted_iota(jnp.int32, pos.shape, 1) + (base + start)
            part = jnp.where(
                (key >= low) & (key <= pos), s[:, h * HEAD_SIZE : (h + 1) * HEAD_SIZE], MASKED
            )
            s_ref[i, :, h * HEAD_SIZE : (h + 1) * HEAD_SIZE] = part
            top = jnp.maximum(top, part)
        m_ref[...] = top
        return carry

    lax.fori_loop(0, chunks, score_step, 0, unroll=True)
    top = jnp.max(m_ref[...], axis=1, keepdims=True) * SCORE_TO_LOG2
    top = jnp.maximum(top, NO_TOP).astype(jnp.bfloat16).astype(jnp.float32)
    top = jnp.broadcast_to(top, m_ref.shape)
    m_ref[...] = top

    def weigh_step(i, carry):
        at = pl.multiple_of(i * chunk_rows, chunk_rows)
        tops = jnp.concatenate([m_ref[...]] * (chunk_rows // HEAD_SIZE), axis=1)
        p = jnp.exp2(s_ref[i] * SCORE_TO_LOG2 - tops).astype(jnp.bfloat16)
        acc_ref[...] += jnp.dot(
            p, v_ref[pl.ds(at, chunk_rows), :], preferred_element_type=jnp.float32
        )
        return carry

    lax.fori_loop(0, chunks, weigh_step, 0, unroll=True)
    tops, totals = [], []
    for g in range(GROUP):
        at = slice(g * each, (g + 1) * each)
        out_ref[:, :, g * HEAD_SIZE : (g + 1) * HEAD_SIZE] = (
            acc_ref[at, :HEAD_SIZE].reshape(peers, EXTRA, HEAD_SIZE).astype(jnp.bfloat16)
        )
        tops.append(m_ref[at])
        totals.append(acc_ref[at, HEAD_SIZE:])
    out_ref[:, :, GROUP * HEAD_SIZE :] = stats_of(tops, totals).reshape(peers, EXTRA, HEAD_SIZE)


def chosen_attention(meta, q_all, kv_all):
    peers, tall, width = q_all.shape
    half = tall - EXTRA
    chunk_rows = 4 * half
    keys = chunk_rows * len(kv_all)
    lines = GROUP * peers * EXTRA
    wide = width + HEAD_SIZE
    return pl.pallas_call(
        chosen_kernel,
        grid_spec=pltpu.PrefetchScalarGridSpec(
            num_scalar_prefetch=1,
            grid=(1,),
            in_specs=[pl.BlockSpec((peers, EXTRA, width), lambda j, meta: (0, half // EXTRA, 0))]
            + [pl.BlockSpec((2, 2, half, 2 * HEAD_SIZE), lambda j, meta: (0, 0, 0, 0))]
            * len(kv_all),
            out_specs=pl.BlockSpec((peers, EXTRA, wide), lambda j, meta: (0, 0, 0)),
            scratch_shapes=[
                pltpu.VMEM((keys, HEAD_SIZE), jnp.bfloat16),
                pltpu.VMEM((keys, 2 * HEAD_SIZE), jnp.bfloat16),
                pltpu.VMEM((lines, HEAD_SIZE), jnp.float32),
                pltpu.VMEM((lines, 2 * HEAD_SIZE), jnp.float32),
                pltpu.VMEM((keys // chunk_rows, lines, chunk_rows), jnp.float32),
            ],
        ),
        out_shape=jax.ShapeDtypeStruct((peers, EXTRA, wide), jnp.bfloat16),
        name="chosen_attention",
    )(meta, q_all, *kv_all)


def attention_kernel(first_block, meta_ref, q_ref, *refs):
    groups = len(refs) - 7
    kv_refs = refs[:groups]
    out_ref, k_ref, v_ref, m_ref, acc_ref, s_ref = refs[groups + 1 :]
    j = pl.program_id(0) + first_block
    half = out_ref.shape[1]
    rows = 2 * half
    chunk_rows = s_ref.shape[3]
    chunks = s_ref.shape[1]
    y, z = meta_ref[DOCS + 1], meta_ref[DOCS + 2]
    span = groups * rows

    @pl.when(j == first_block)
    def _():
        gather_keys(meta_ref, kv_refs, k_ref, v_ref)

    first_q = (2 * j + y) * span + z * rows
    last_q = first_q + rows - 1
    far = span // 2
    reach = far + rows - 1

    chunk_base = functools.partial(chunk_start, meta_ref, groups, rows)
    low_first = doc_start(meta_ref, first_q)
    low_last = doc_start(meta_ref, last_q)
    m_ref[...] = jnp.full(m_ref.shape, NO_TOP, jnp.float32)
    acc_ref[...] = jnp.zeros(acc_ref.shape, jnp.float32)
    chunk_lo, chunk_hi = jnp.int32(0), jnp.int32(0)
    for i in range(chunks):
        base = chunk_base(i)
        chunk_lo += (base + reach < low_first).astype(jnp.int32)
        chunk_hi += (base <= last_q).astype(jnp.int32)

    def score(i, masked):
        at = pl.multiple_of(i * chunk_rows, chunk_rows)
        k = k_ref[pl.ds(at, chunk_rows), :]
        if masked:
            pos = first_q + lax.broadcasted_iota(jnp.int32, (rows, 1), 0)
            low = doc_start(meta_ref, pos)
            base = chunk_base(i)
            key = lax.broadcasted_iota(jnp.int32, (rows, chunk_rows), 1)
            key = key + jnp.where(key >= rows, far - rows, 0)
            allowed = (key >= low - base) & (key <= pos - base)
        for g in range(GROUP):
            q = q_ref[:, :, g * HEAD_SIZE : (g + 1) * HEAD_SIZE].reshape(rows, HEAD_SIZE)
            s = lax.dot_general(
                q, k, (((1,), (1,)), ((), ())), preferred_element_type=jnp.float32
            )
            if masked:
                s = jnp.where(allowed, s, MASKED)
            s_ref[g, i] = s
            top = m_ref[g]
            for h in range(chunk_rows // HEAD_SIZE):
                top = jnp.maximum(top, s[:, h * HEAD_SIZE : (h + 1) * HEAD_SIZE])
            m_ref[g] = top

    def score_step(i, carry):
        base = chunk_base(i)
        free = (base >= low_last) & (base + reach <= first_q)

        @pl.when(free)
        def _():
            score(i, False)

        @pl.when(jnp.logical_not(free))
        def _():
            score(i, True)

        return carry

    lax.fori_loop(chunk_lo, chunk_hi, score_step, 0)
    for g in range(GROUP):
        top = jnp.max(m_ref[g], axis=1, keepdims=True) * SCORE_TO_LOG2
        top = jnp.maximum(top, NO_TOP).astype(jnp.bfloat16).astype(jnp.float32)
        m_ref[g] = jnp.broadcast_to(top, (rows, HEAD_SIZE))

    def weigh_step(i, carry):
        at = pl.multiple_of(i * chunk_rows, chunk_rows)
        v = v_ref[pl.ds(at, chunk_rows), :]
        for g in range(GROUP):
            top = m_ref[g]
            top = jnp.concatenate([top] * (chunk_rows // HEAD_SIZE), axis=1)
            p = jnp.exp2(s_ref[g, i] * SCORE_TO_LOG2 - top).astype(jnp.bfloat16)
            acc_ref[g] += jnp.dot(p, v, preferred_element_type=jnp.float32)
        return carry

    lax.fori_loop(chunk_lo, chunk_hi, weigh_step, 0)

    for g in range(GROUP):
        out_ref[:, :, g * HEAD_SIZE : (g + 1) * HEAD_SIZE] = (
            acc_ref[g, :, :HEAD_SIZE].astype(jnp.bfloat16).reshape(2, half, HEAD_SIZE)
        )
    stats = stats_of(
        [m_ref[g] for g in range(GROUP)], [acc_ref[g, :, HEAD_SIZE:] for g in range(GROUP)]
    )
    out_ref[:, :, GROUP * HEAD_SIZE :] = stats.reshape(2, half, HEAD_SIZE)


def partial_attention(meta, q_all, kv_all, first, number, before):
    peers, tall, width = q_all.shape
    half = tall - EXTRA
    rows = 2 * half
    chunk_rows = 2 * rows
    keys = chunk_rows * len(kv_all)
    wide = width + HEAD_SIZE
    at = lambda j, meta: (j + first, 0, 0)
    return pl.pallas_call(
        functools.partial(attention_kernel, first),
        grid_spec=pltpu.PrefetchScalarGridSpec(
            num_scalar_prefetch=1,
            grid=(number,),
            in_specs=[pl.BlockSpec((2, half, width), at)]
            + [pl.BlockSpec((2, 2, half, 2 * HEAD_SIZE), lambda j, meta: (0, 0, 0, 0))]
            * len(kv_all)
            + [pl.BlockSpec(memory_space=pl.ANY)],
            out_specs=pl.BlockSpec((2, half, wide), at),
            scratch_shapes=[
                pltpu.VMEM((keys, HEAD_SIZE), jnp.bfloat16),
                pltpu.VMEM((keys, 2 * HEAD_SIZE), jnp.bfloat16),
                pltpu.VMEM((GROUP, rows, HEAD_SIZE), jnp.float32),
                pltpu.VMEM((GROUP, rows, 2 * HEAD_SIZE), jnp.float32),
                pltpu.VMEM((GROUP, keys // chunk_rows, rows, chunk_rows), jnp.float32),
            ],
        ),
        out_shape=jax.ShapeDtypeStruct((peers, half, wide), jnp.bfloat16),
        input_output_aliases={2 + len(kv_all): 0} if first else {},
        compiler_params=pltpu.CompilerParams(dimension_semantics=("arbitrary",)),
        cost_estimate=pl.CostEstimate(
            flops=number * 5 * 10**9, bytes_accessed=4 * 10**6, transcendentals=0
        ),
        name="partial_attention",
    )(meta, q_all, *kv_all, before)


def merge_parts(parts_ref, merged_ref):
    windows = parts_ref.shape[0] // 2
    rows = parts_ref.shape[1]
    for c in range(2):
        tops, sums = [], []
        for w in range(windows):
            st = parts_ref[2 * w + c, :, GROUP * HEAD_SIZE :].astype(jnp.float32)
            tops.append(st)
            sums.append(
                pltpu.roll(st, HEAD_SIZE - GROUP, 1)
                + pltpu.roll(st, HEAD_SIZE - 2 * GROUP, 1)
                + pltpu.roll(st, HEAD_SIZE - 3 * GROUP, 1)
            )
        top = functools.reduce(jnp.maximum, tops)
        shares = [jnp.exp2(t - top) for t in tops]
        total = functools.reduce(jnp.add, [n * share for n, share in zip(sums, shares)])
        lane = lax.broadcasted_iota(jnp.int32, total.shape, 1)
        total = jnp.where((lane < GROUP) & (total > 0.0), total, 1.0)
        shares = [share / total for share in shares]
        for g in range(GROUP):
            result = jnp.zeros((rows, HEAD_SIZE), jnp.float32)
            for w in range(windows):
                part = parts_ref[2 * w + c, :, g * HEAD_SIZE : (g + 1) * HEAD_SIZE]
                result = result + shares[w][:, g : g + 1] * part.astype(jnp.float32)
            at = (c * GROUP + g) * HEAD_SIZE
            merged_ref[:, at : at + HEAD_SIZE] = result.astype(jnp.bfloat16)


def merge_kernel(parts_ref, merged_ref):
    merge_parts(parts_ref, merged_ref)


def project_kernel(parts_ref, *refs):
    weight_refs = refs[:-3]
    out_ref, merged_ref, chosen_ref = refs[-3:]
    n = pl.program_id(0)
    heads = chosen_ref.shape[0]

    @pl.when(n == 0)
    def _():
        merge_parts(parts_ref, merged_ref)
        for head in range(heads):
            chosen_ref[head] = merged_ref[:, head * HEAD_SIZE : (head + 1) * HEAD_SIZE]
        out_ref[...] = jnp.zeros(out_ref.shape, jnp.float32)

    product = 0.0
    for k, weight_ref in enumerate(weight_refs):
        product = product + jnp.dot(
            chosen_ref[n * len(weight_refs) + k],
            weight_ref[...],
            preferred_element_type=jnp.float32,
        )
    out_ref[...] += product[: out_ref.shape[0]]


def projected_rows(parts, out_weight, count):
    rows = parts.shape[1]
    features, width = out_weight.shape
    heads = features // HEAD_SIZE
    streams = 4
    return pl.pallas_call(
        project_kernel,
        grid=(heads // streams,),
        in_specs=[pl.BlockSpec(parts.shape, lambda n: (0, 0, 0))]
        + [
            pl.BlockSpec((HEAD_SIZE, width), functools.partial(lambda k, n: (n * streams + k, 0), k))
            for k in range(streams)
        ],
        out_specs=pl.BlockSpec((count, width), lambda n: (0, 0)),
        out_shape=jax.ShapeDtypeStruct((count, width), jnp.float32),
        scratch_shapes=[
            pltpu.VMEM((rows, features), jnp.bfloat16),
            pltpu.VMEM((heads, rows, HEAD_SIZE), jnp.bfloat16),
        ],
        compiler_params=pltpu.CompilerParams(dimension_semantics=("arbitrary",)),
        name="projected_rows",
    )(parts, *[out_weight] * streams)


def merged_attention(parts):
    rows = parts.shape[1]
    return pl.pallas_call(
        merge_kernel,
        in_specs=[pl.BlockSpec(memory_space=pltpu.VMEM)],
        out_specs=pl.BlockSpec(memory_space=pltpu.VMEM),
        out_shape=jax.ShapeDtypeStruct((rows, 2 * GROUP * HEAD_SIZE), jnp.bfloat16),
        name="merged_attention",
    )(parts)


def merged_stats(stats, axis):
    tops, sums, targets = stats
    top = jnp.max(tops, axis=axis)
    total = jnp.sum(sums * jnp.exp(tops - jnp.expand_dims(top, axis)), axis=axis)
    return (top, total, jnp.sum(targets, axis=axis))


def per_device(
    queries,
    rotated_keys,
    value_matrix,
    doc_lengths,
    scored,
    residual,
    norm_gain,
    out_weight,
    lm_weight,
    token_ids,
    old_logp,
    advantage,
):
    tok_rows = queries.shape[0]
    count = scored.shape[0]
    nx, ny, nz, cores = [lax.axis_size(a) for a in CTX]
    x, y, z, core = [lax.axis_index(a) for a in CTX]
    doc_starts = jnp.cumsum(doc_lengths) - doc_lengths
    meta = jnp.concatenate(
        [doc_starts.astype(jnp.int32), jnp.stack([x, y, z, core]).astype(jnp.int32)]
    )

    def of_head(c):
        at = c * HEAD_SIZE
        return jnp.concatenate(
            [
                lax.dynamic_slice_in_dim(rotated_keys, at, HEAD_SIZE, 1),
                lax.dynamic_slice_in_dim(value_matrix, at, HEAD_SIZE, 1),
            ],
            axis=1,
        )

    def handed(dy, dc):
        return [
            (
                ((i * ny + k) * nz + l) * cores + c,
                ((((i + l) % nx) * ny + (k ^ dy)) * nz + l) * cores + (c ^ dc),
            )
            for i in range(nx)
            for k in range(ny)
            for l in range(nz)
            for c in range(cores)
        ]

    mine, others = of_head(core), of_head(1 - core)
    pieces = []
    for dy in range(ny):
        for dc in range(cores):
            pieces.append(lax.ppermute(others if dc else mine, CTX, handed(dy, dc)))
    own = jnp.stack(pieces).reshape(ny, cores, tok_rows, 2 * HEAD_SIZE)

    def shifted(a, d):
        return lax.ppermute(a, "ctx_2", [(k, (k + d) % nz) for k in range(nz)])

    far = nz // 2
    kv_all = [own] + [None] * (nz - 1)
    for d in range(1, far):
        kv_all[d] = shifted(kv_all[d - 1], 1)
        kv_all[nz - d] = shifted(kv_all[(nz - d + 1) % nz], -1)
    kv_all[far] = jnp.stack([shifted(kv_all[far - 1][0], 1), shifted(kv_all[far + 1][1], -1)])
    q_send = queries_to_send(scored, queries, nx)
    q_all = lax.all_to_all(q_send, XC, 0, 0, tiled=True)
    few = chosen_attention(meta, q_all, kv_all)
    few = lax.all_to_all(few, XC, 0, 0, tiled=True)
    partial_value = projected_rows(few, out_weight, count)
    parts = q_all
    for first, number in ((0, 2), (2, nx - 2)):
        parts = partial_attention(meta, q_all, kv_all, first, number, parts)
    arrived = lax.all_to_all(parts, XC, 0, 0, tiled=True)
    attended = merged_attention(arrived)

    half = residual.shape[1]
    head = lax.axis_index("head")
    own = lax.dynamic_slice_in_dim(partial_value, head * half, half, 1)
    own = own + residual.astype(jnp.float32)
    partial_value = lax.dynamic_update_slice_in_dim(partial_value, own, head * half, 1)
    other = swap_heads(partial_value.astype(jnp.bfloat16)).astype(jnp.float32)
    hidden_all = partial_value + other
    squares = jnp.sum(hidden_all * hidden_all, axis=1, keepdims=True)
    hidden = own + lax.dynamic_slice_in_dim(other, head * half, half, 1)
    normed = (
        hidden * lax.rsqrt(squares / hidden_all.shape[1] + 1e-05) * norm_gain[None, :]
    ).astype(jnp.bfloat16)

    along_yz = spread(normed, YZ)
    own_rows = spread(along_yz, ("ctx_0",)).reshape(-1, half)
    other_rows = lax.ppermute(own_rows, "ctx_3", [(0, 1), (1, 0)])
    rows = own_rows.shape[0] // 2
    chips = nx * ny * nz
    vocab_rows = lm_weight.shape[1]
    my_index = ((x * ny + y) * nz + z) * cores + core
    ids = token_ids.reshape(chips, cores, count).swapaxes(0, 1).reshape(cores, 2, rows)
    ids = lax.dynamic_index_in_dim(ids, head, 1, keepdims=False) - my_index * vocab_rows

    def local_stats(normed_rows, local_ids):
        partial_logits = jnp.dot(
            normed_rows, lm_weight, preferred_element_type=jnp.float32
        )
        theirs = lax.dynamic_slice_in_dim(partial_logits, (1 - head) * rows, rows, 0)
        ours = lax.dynamic_slice_in_dim(partial_logits, head * rows, rows, 0)
        theirs = swap_heads(theirs.astype(jnp.bfloat16))
        logits = ours + theirs.astype(jnp.float32)
        matches = local_ids[:, None] == jnp.arange(vocab_rows, dtype=jnp.int32)[None, :]
        target_part = jnp.sum(jnp.where(matches, logits, 0.0), axis=1)
        local_top = jnp.max(logits, axis=1)
        sum_part = jnp.sum(jnp.exp(logits - local_top[:, None]), axis=1)
        return jnp.stack([local_top, sum_part, target_part])

    ids_first = lax.dynamic_index_in_dim(ids, core, 0, keepdims=False)
    ids_second = lax.dynamic_index_in_dim(ids, 1 - core, 0, keepdims=False)
    first = local_stats(own_rows, ids_first)
    second = local_stats(other_rows, ids_second)
    stats = jnp.where(core == 0, jnp.stack([first, second]), jnp.stack([second, first]))
    by_z = spread(stats, ("ctx_2",))
    merged = merged_stats((by_z[:, :, 0], by_z[:, :, 1], by_z[:, :, 2]), 0)
    by_rest = spread(jnp.stack(merged), XYCH)
    by_rest = by_rest.reshape(-1, 2, 3, cores, rows)
    top, total, target = merged_stats((by_rest[:, :, 0], by_rest[:, :, 1], by_rest[:, :, 2]), 0)
    log_probs = (target - top - jnp.log(total)).reshape(2, cores, rows // count, count)
    log_probs = log_probs.swapaxes(1, 2).reshape(chips * cores * count)
    ratio = jnp.exp(jnp.clip(log_probs - old_logp, -4.0, 4.0))
    token_loss = -jnp.minimum(ratio * advantage, jnp.clip(ratio, 0.8, 1.2) * advantage)
    return (attended, log_probs, token_loss)


def solution(mesh):
    finer = Mesh(mesh.devices.reshape(4, 2, 8, 2, mesh.shape["head"]), AXES)
    ctx = AXES[:4]
    placed = (
        P(ctx, "head"),
        P(ctx, "head"),
        P(ctx, "head"),
        P(),
        P(ctx),
        P(ctx, "head"),
        P("head"),
        P("head", None),
        P("head", ctx),
        P(),
        P(),
        P(),
    )

    return jax.shard_map(
        per_device,
        mesh=finer,
        in_specs=placed,
        out_specs=(P(ctx, "head"), P(), P()),
        check_vma=False,
    )
```
